32 devices in a mesh: tp: 4 (over z), cp: 8 (over y, x, core).
Axes of the slice: x: 2, y: 2, z: 4, core: 2. Of those that a mesh axis runs over, the one named last changes fastest.
Arguments:
- q_raw: bfloat16 [4096, 16, 128], P('cp', 'tp'), parts along dimension 1
- k_raw: bfloat16 [4096, 8, 128], P('cp', 'tp'), parts along dimension 1
- v_raw: bfloat16 [4096, 8, 128], P('cp', 'tp'), parts along dimension 1
- positions: int32 [4096], P('cp')
- seq_ids: int32 [4096], P('cp')
- q_gain: bfloat16 [128], replicated
- k_gain: bfloat16 [128], replicated
Outputs:
- output 1: bfloat16 [4096, 16, 128], P('cp', 'tp'), parts along dimension 1
- output 2: float32 [4096, 16], P('cp', 'tp'), parts along dimension 1
There are 4 independent parts. The reference program is written for one: setup_inputs(seed, part) draws one part's arguments, and reference() takes and returns one part's arrays. A program takes and returns all parts, laid end to end along the dimension named above; an argument that names none is the same for every part.
All inputs are finite; a program needn't handle non-finite values.
Results may differ from the reference program's by a relative error of at most 0.017719.
Values are sent between devices in bfloat16 or wider.
A program may use at most 1 GiB of HBM per device.

```python
import jax
import jax.numpy as jnp
from jax import lax

N_TOKENS = 4096
PART_Q_HEADS = 4
PART_KV_HEADS = 2
HEAD_DIM = 128
CP_SIZE = 8
SEQ_COUNT = 4
ROW_BLOCK = 64
THETA = 1000000.0
EPS = 1e-6
NEG_BIG = -1e30


def draw_layout(key):
    units = N_TOKENS // (2 * CP_SIZE)
    picks = jax.random.permutation(key, units - 1)[: SEQ_COUNT - 1] + 1
    cuts = jnp.sort(picks).astype(jnp.int32)
    bounds = jnp.concatenate([jnp.zeros((1,), jnp.int32), cuts, jnp.full((1,), units, jnp.int32)])
    lengths = bounds[1:] - bounds[:-1]
    local_idx = jnp.arange(2 * units, dtype=jnp.int32)
    seq_local = jnp.sum((local_idx[:, None] >= 2 * cuts[None, :]).astype(jnp.int32), axis=1)
    piece_len = lengths[seq_local]
    within = local_idx - 2 * bounds[seq_local]
    first_half = within < piece_len
    device_idx = jnp.arange(CP_SIZE, dtype=jnp.int32)[:, None]
    piece_idx = jnp.where(first_half[None, :], device_idx, 2 * CP_SIZE - 1 - device_idx)
    offset = jnp.where(first_half, within, within - piece_len)
    positions = piece_idx * piece_len[None, :] + offset[None, :]
    seq_ids = jnp.broadcast_to(seq_local[None, :], (CP_SIZE, 2 * units))
    return positions.reshape(N_TOKENS).astype(jnp.int32), seq_ids.reshape(N_TOKENS).astype(jnp.int32)


def setup_inputs(seed: int = 0, part: int = 0) -> dict:
    key = jax.random.key(seed)
    key_layout, key_gq, key_gk, key_vals = jax.random.split(key, 4)
    positions, seq_ids = draw_layout(key_layout)
    part_key = jax.random.fold_in(key_vals, part)
    key_q, key_k, key_v = jax.random.split(part_key, 3)
    q_raw = jax.random.normal(key_q, (N_TOKENS, PART_Q_HEADS, HEAD_DIM), jnp.float32).astype(jnp.bfloat16)
    k_raw = jax.random.normal(key_k, (N_TOKENS, PART_KV_HEADS, HEAD_DIM), jnp.float32).astype(jnp.bfloat16)
    v_raw = jax.random.normal(key_v, (N_TOKENS, PART_KV_HEADS, HEAD_DIM), jnp.float32).astype(jnp.bfloat16)
    q_gain = (1.3 + 0.4 * jax.random.normal(key_gq, (HEAD_DIM,), jnp.float32)).astype(jnp.bfloat16)
    k_gain = (1.3 + 0.4 * jax.random.normal(key_gk, (HEAD_DIM,), jnp.float32)).astype(jnp.bfloat16)
    return {"q_raw": q_raw, "k_raw": k_raw, "v_raw": v_raw, "positions": positions, "seq_ids": seq_ids, "q_gain": q_gain, "k_gain": k_gain}


def norm_rope(x_in, gain, positions):
    head_dim = x_in.shape[-1]
    half = head_dim // 2
    x_f32 = x_in.astype(jnp.float32)
    inv_rms = lax.rsqrt(jnp.mean(x_f32 * x_f32, axis=-1, keepdims=True) + EPS)
    normed = (x_f32 * inv_rms * gain.astype(jnp.float32)).astype(jnp.bfloat16).astype(jnp.float32)
    inv_freq = jnp.power(THETA, -(jnp.arange(half, dtype=jnp.float32) * 2.0) / head_dim)
    angle = positions.astype(jnp.float32)[:, None] * inv_freq[None, :]
    cos_a = jnp.cos(angle)[:, None, :]
    sin_a = jnp.sin(angle)[:, None, :]
    first = normed[..., :half]
    second = normed[..., half:]
    rotated = jnp.concatenate([first * cos_a - second * sin_a, second * cos_a + first * sin_a], axis=-1)
    return rotated.astype(jnp.bfloat16)


def reference(q_raw, k_raw, v_raw, positions, seq_ids, q_gain, k_gain):
    group = PART_Q_HEADS // PART_KV_HEADS
    scale = HEAD_DIM ** -0.5
    q_rot = norm_rope(q_raw, q_gain, positions)
    k_all = norm_rope(k_raw, k_gain, positions).astype(jnp.float32)
    v_all = v_raw.astype(jnp.float32)
    n_blocks = N_TOKENS // ROW_BLOCK
    q_blocks = q_rot.reshape(n_blocks, ROW_BLOCK, PART_KV_HEADS, group, HEAD_DIM)
    pos_blocks = positions.reshape(n_blocks, ROW_BLOCK)
    seq_blocks = seq_ids.reshape(n_blocks, ROW_BLOCK)

    def one_block(block_in):
        q_blk, q_pos, q_seq = block_in
        scores = jnp.einsum("rkgd,skd->rkgs", q_blk.astype(jnp.float32), k_all) * scale
        allowed = (q_seq[:, None] == seq_ids[None, :]) & (positions[None, :] <= q_pos[:, None])
        scores = jnp.where(allowed[:, None, None, :], scores, NEG_BIG)
        row_max = jnp.max(scores, axis=-1)
        weights = jnp.exp(scores - row_max[..., None])
        row_sum = jnp.sum(weights, axis=-1)
        attn_blk = jnp.einsum("rkgs,skd->rkgd", weights, v_all) / row_sum[..., None]
        log_sum = row_max + jnp.log(row_sum)
        return attn_blk.astype(jnp.bfloat16).reshape(ROW_BLOCK, PART_Q_HEADS, HEAD_DIM), log_sum.reshape(ROW_BLOCK, PART_Q_HEADS)

    attn_blocks, log_blocks = lax.map(one_block, (q_blocks, pos_blocks, seq_blocks))
    return attn_blocks.reshape(N_TOKENS, PART_Q_HEADS, HEAD_DIM), log_blocks.reshape(N_TOKENS, PART_Q_HEADS)
```

```python
import functools
import math

import jax
import jax.numpy as jnp
import numpy as np
from jax import lax
from jax.experimental import pallas as pl
from jax.experimental.pallas import tpu as pltpu
from jax.sharding import PartitionSpec as P

THETA = 1000000.0
EPS = 1e-6
NEG_BIG = -1e30
D = 128
HALF = 256
ROWS = 512
C_EXP = (D ** -0.5) * math.log2(math.e)
SCALE = D ** -0.5
F32 = jnp.float32
BF16 = jnp.bfloat16


def nt(a, b):
    return lax.dot_general(a, b, (((1,), (1,)), ((), ())), preferred_element_type=F32)


def nn(a, b):
    return lax.dot_general(a, b, (((1,), (0,)), ((), ())), preferred_element_type=F32)


def kernel(q_hbm, k_hbm, v_hbm, pos_hbm, seq_hbm, qg_hbm, kg_hbm, freq_hbm, out_hbm, lse_hbm,
           q_in, k_in, v_in, pos_v, seq_v, qg_v, kg_v, freq_v, f_scr, cs_scr, perm, perm_t,
           kbuf, vbuf, kst, vst, qbuf, qst, kaug, m_scr, l_scr, acc, ost, obuf, lst, lbuf, out_v, lse_v,
           in_sem, out_sem, s_kx, s_vx, s_p, s_q, s_fk, s_fv, s_o, s_l, r_k, r_v, r_q, r_o, r_l):
    me = lax.axis_index("cp")
    core = lax.rem(me, 2)
    chip = lax.div(me, 2)
    x = lax.rem(chip, 2)
    y = lax.div(chip, 2)
    xchip = chip + 1 - 2 * x
    ychip = chip + 2 - 4 * y
    other = 1 - core
    partner = 2 * chip + other

    def rcopy(src, dst, ssem, rsem, dev):
        return pltpu.make_async_remote_copy(src_ref=src, dst_ref=dst, send_sem=ssem, recv_sem=rsem,
                                            device_id={"cp": dev}, device_id_type=pl.DeviceIdType.MESH)

    ins = [(v_hbm, v_in), (seq_hbm, seq_v), (pos_hbm, pos_v), (k_hbm, k_in), (kg_hbm, kg_v), (freq_hbm, freq_v),
           (q_hbm, q_in), (qg_hbm, qg_v)]
    in_copies = [pltpu.make_async_copy(src, dst, in_sem.at[n]) for n, (src, dst) in enumerate(ins)]
    for cp in in_copies:
        cp.start()
    barrier = pltpu.get_barrier_semaphore()
    peers = [partner, 2 * xchip, 2 * xchip + 1, 2 * ychip, 2 * ychip + 1]
    for peer in peers:
        pl.semaphore_signal(barrier, inc=1, device_id={"cp": peer}, device_id_type=pl.DeviceIdType.MESH)

    in_copies[1].wait()
    seq = seq_v[...]
    row_id = lax.broadcasted_iota(jnp.int32, (8, ROWS), 1).astype(F32)
    sub_id = lax.broadcasted_iota(jnp.int32, (8, ROWS), 0)
    is_seq = jnp.broadcast_to(seq, (8, ROWS)) == sub_id
    seq_f = jnp.where(is_seq, 1.0, 0.0)
    cnt = jnp.sum(seq_f, axis=1, keepdims=True)
    start = jnp.min(jnp.where(is_seq, row_id, float(ROWS)), axis=1, keepdims=True)
    start_row = jnp.sum(seq_f * start, axis=0, keepdims=True)
    cnt_row = jnp.sum(seq_f * cnt, axis=0, keepdims=True)
    off = row_id[:1] - start_row
    late = off * 2.0 >= cnt_row
    dest = start_row * 0.5 + off + jnp.where(late, HALF - 0.5 * cnt_row, 0.0)
    dest_i = dest.astype(jnp.int32)
    for blk in range(4):
        rows = lax.broadcasted_iota(jnp.int32, (128, ROWS), 0) + blk * 128
        perm[pl.ds(blk * 128, 128), :] = jnp.where(rows == dest_i, 1.0, 0.0).astype(BF16)

    in_copies[0].wait()
    f_scr[pl.ds(0, 1024), :] = v_in[...].astype(F32)
    for h in range(2):
        vt = f_scr[pl.ds(h, ROWS, stride=2), :].T.astype(BF16)
        vc = nt(vt, perm[...]).astype(BF16)
        for half in range(2):
            vst[h, half] = vc[:, half * HALF:(half + 1) * HALF]
    for half in range(2):
        vbuf[0, half, core] = vst[core, half]
    pl.semaphore_wait(barrier, 5)

    sends = []
    for half in range(2):
        for h in range(2):
            for t, tchip in enumerate((xchip, ychip)):
                sends.append(rcopy(vst.at[h, half], vbuf.at[1 + t, half, core], s_vx.at[t, h, half],
                                   r_v.at[1 + t, core, half], 2 * tchip + h))
                sends[-1].start()
    for half in range(2):
        sends.append(rcopy(vst.at[other, half], vbuf.at[0, half, core], s_p.at[0, half], r_v.at[0, core, half], partner))
        sends[-1].start()

    in_copies[2].wait()
    in_copies[5].wait()
    angle = freq_v[...] * pos_v[...].astype(F32)
    cs_scr[0] = jnp.cos(angle)
    cs_scr[1] = jnp.sin(angle)

    def norm_rope(rows_f32, gain_v):
        xt = rows_f32.T
        inv = lax.rsqrt(jnp.mean(xt * xt, axis=0, keepdims=True) + EPS)
        gain = jnp.broadcast_to(gain_v[...].astype(F32), (128, D)).T
        gain = jnp.concatenate([gain] * 4, axis=1)
        n = (xt * inv * gain).astype(BF16).astype(F32)
        a, b = n[:64], n[64:]
        cos, sin = cs_scr[0], cs_scr[1]
        return jnp.concatenate([a * cos - b * sin, b * cos + a * sin], axis=0).astype(BF16)

    in_copies[3].wait()
    in_copies[4].wait()
    f_scr[pl.ds(0, 1024), :] = k_in[...].astype(F32)
    for h in range(2):
        kr = norm_rope(f_scr[pl.ds(h, ROWS, stride=2), :], kg_v)
        kc = nt(perm[...], kr).astype(BF16)
        for half in range(2):
            kst[h, half] = kc[half * HALF:(half + 1) * HALF, :]
    for half in range(2):
        kbuf[0, half, core] = kst[core, half]

    for half in range(2):
        for h in range(2):
            for t, tchip in enumerate((xchip, ychip)):
                sends.append(rcopy(kst.at[h, half], kbuf.at[1 + t, half, core], s_kx.at[t, h, half],
                                   r_k.at[1 + t, core, half], 2 * tchip + h))
                sends[-1].start()
    for half in range(2):
        sends.append(rcopy(kst.at[other, half], kbuf.at[0, half, core], s_p.at[1, half], r_k.at[0, core, half], partner))
        sends[-1].start()

    in_copies[6].wait()
    in_copies[7].wait()
    f_scr[...] = q_in[...].astype(F32)

    def q_head(h, store):
        qr = norm_rope(f_scr[pl.ds(h, ROWS, stride=4), :], qg_v)
        qc = nt(qr, perm[...]).astype(BF16)
        for half in range(2):
            store(half, qc[:, half * HALF:(half + 1) * HALF])

    for g in range(2):
        def store_other(half, val, g=g):
            qst[half, :, g * HALF:(g + 1) * HALF] = val
        q_head(2 * other + g, store_other)
    for half in range(2):
        sends.append(rcopy(qst.at[half], qbuf.at[half, 0, pl.ds(0, D), :], s_q.at[half], r_q.at[half], partner))
        sends[-1].start()
    for g in range(2):
        def store_own(half, val, g=g):
            qbuf[half, 1, pl.ds(0, D), g * HALF:(g + 1) * HALF] = val
        q_head(2 * core + g, store_own)

    lane_d = lax.broadcasted_iota(jnp.int32, (8, HALF), 1).astype(F32)
    in_run = (lane_d >= start * 0.5) & (lane_d < (start + cnt) * 0.5)
    one_hot = jnp.where(in_run, 1.0, 0.0)
    blocked = jnp.where(in_run, 0.0, NEG_BIG)
    blocked = jnp.where(lax.broadcasted_iota(jnp.int32, (8, HALF), 0) < 4, blocked, 0.0)
    pad = jnp.zeros((D - 8, HALF), F32)
    q_extra = jnp.concatenate([blocked, pad], axis=0).astype(BF16)
    for half in range(2):
        for dev in range(2):
            for g in range(2):
                qbuf[half, dev, pl.ds(D, D), g * HALF:(g + 1) * HALF] = q_extra
    kaug[...] = jnp.concatenate([one_hot, pad], axis=0).T.astype(BF16)

    dest_cols = jnp.broadcast_to(dest, (128, ROWS)).T.astype(jnp.int32)
    for blk in range(4):
        lanes = lax.broadcasted_iota(jnp.int32, (ROWS, 128), 1) + blk * 128
        perm_t[:, blk * 128:(blk + 1) * 128] = jnp.where(lanes == dest_cols, 1.0, 0.0).astype(BF16)

    m_scr[...] = jnp.full(m_scr.shape, NEG_BIG, F32)
    l_scr[...] = jnp.zeros(l_scr.shape, F32)
    acc[...] = jnp.zeros(acc.shape, F32)

    def tile(slot, khalf, qhalf, causal):
        keys = kbuf[slot, khalf].reshape(2 * HALF, D)
        ka = kaug[...]
        keys = jnp.concatenate([keys, jnp.concatenate([ka, ka], axis=0)], axis=1)
        v0 = vbuf[slot, khalf, 0]
        v1 = vbuf[slot, khalf, 1]
        for dev in range(2):
            for g in range(2):
                cols = pl.ds(g * HALF, HALF)
                s = nn(keys, qbuf[qhalf, dev, :, cols])
                if causal:
                    abs_dev = core if dev == 1 else other
                    krow = lax.broadcasted_iota(jnp.int32, (2 * HALF, HALF), 0)
                    qcol = lax.broadcasted_iota(jnp.int32, (2 * HALF, HALF), 1)
                    kord = krow + qhalf * jnp.where(krow < HALF, HALF, -HALF)
                    qord = qcol + (abs_dev + qhalf * (1 - 2 * abs_dev)) * HALF
                    s = jnp.where(kord <= qord, s, NEG_BIG)
                m_old = m_scr[qhalf, dev, :, cols]
                m_new = jnp.maximum(m_old, jnp.max(s, axis=0, keepdims=True))
                p = jnp.exp2((s - m_new) * C_EXP)
                alpha = jnp.exp2((m_old - m_new) * C_EXP)
                m_scr[qhalf, dev, :, cols] = m_new
                l_scr[qhalf, dev, :, cols] = l_scr[qhalf, dev, :, cols] * alpha + jnp.sum(p, axis=0, keepdims=True)
                pb = p.astype(BF16)
                o = nn(v0, pb[:HALF]) + nn(v1, pb[HALF:])
                acc[qhalf, dev, :, cols] = acc[qhalf, dev, :, cols] * alpha + o

    def got_k(slot, dev, half):
        rcopy(kst.at[0, half], kbuf.at[slot, half, dev], s_kx.at[0, 0, half], r_k.at[slot, dev, half], partner).wait_recv()

    def got_v(slot, dev, half):
        rcopy(vst.at[0, half], vbuf.at[slot, half, dev], s_vx.at[0, 0, half], r_v.at[slot, dev, half], partner).wait_recv()

    for half in range(2):
        got_v(0, other, half)
        got_k(0, other, half)
        rcopy(qst.at[half], qbuf.at[half, 0, pl.ds(0, D), :], s_q.at[half], r_q.at[half], partner).wait_recv()

    def own_body(half, carry):
        tile(0, half, half, True)
        return carry

    lax.fori_loop(0, 2, own_body, 0)

    def fwd_v(dev, half):
        return rcopy(vbuf.at[2, half, dev], vbuf.at[3, half, dev], s_fv.at[dev, half], r_v.at[3, dev, half], 2 * xchip + core)

    def fwd_k(dev, half):
        return rcopy(kbuf.at[1, half, dev], kbuf.at[3, half, dev], s_fk.at[dev, half], r_k.at[3, dev, half], 2 * ychip + core)

    def body(idx, carry):
        grp = (idx + 1) // 2
        second = (idx + 1) % 2

        @pl.when(idx == 1)
        def _():
            for half in range(2):
                for dev in range(2):
                    got_v(2, dev, half)
                    fwd_v(dev, half).start()
            for dev in range(2):
                got_k(1, dev, 0)
                fwd_k(dev, 0).start()
                got_v(1, dev, 0)

        @pl.when(idx == 2)
        def _():
            for dev in range(2):
                got_k(1, dev, 1)
                fwd_k(dev, 1).start()
                got_v(1, dev, 1)

        @pl.when(idx == 3)
        def _():
            for dev in range(2):
                got_k(2, dev, 0)

        @pl.when(idx == 4)
        def _():
            for dev in range(2):
                got_k(2, dev, 1)

        @pl.when(idx == 5)
        def _():
            for dev in range(2):
                got_v(3, dev, 0)
                got_k(3, dev, 0)

        @pl.when(idx == 6)
        def _():
            for dev in range(2):
                got_v(3, dev, 1)
                got_k(3, dev, 1)

        use_x = (4 - grp) // 3
        late_needed = (1 - y) + use_x * (y - x)
        snd = second * ((idx + 6) // 7)
        sel = snd * late_needed
        tile(grp * ((idx + 6) // 7), sel, 1 - snd + sel, False)
        return carry

    lax.fori_loop(0, 7, body, 0)

    def finish(dev, dst_o, dst_l):
        for half in range(2):
            for g in range(2):
                cols = pl.ds(g * HALF, HALF)
                l = l_scr[half, dev, :, cols]
                o = acc[half, dev, :, cols] * (1.0 / l)
                dst_o(half, g, o.astype(BF16))
                dst_l(half, g, m_scr[half, dev, :, cols] * SCALE + jnp.log(l))

    def st_o(half, g, val):
        ost[g, :, half * HALF:(half + 1) * HALF] = val

    def st_l(half, g, val):
        lst[pl.ds(g, 1), half * HALF:(half + 1) * HALF] = val

    finish(0, st_o, st_l)
    o_send = rcopy(ost, obuf.at[core], s_o.at[0], r_o.at[0], partner)
    l_send = rcopy(lst, lbuf.at[core], s_l.at[0], r_l.at[0], partner)
    o_send.start()
    l_send.start()

    def own_o(half, g, val):
        obuf[core, g, :, half * HALF:(half + 1) * HALF] = val

    def own_l(half, g, val):
        lbuf[core, pl.ds(g, 1), half * HALF:(half + 1) * HALF] = val

    finish(1, own_o, own_l)

    def place(grp):
        for g in range(2):
            f_scr[pl.ds(2 * grp + g, ROWS, stride=4), :] = nt(perm_t[...], obuf[grp, g])

    place(core)
    rcopy(ost, obuf.at[other], s_o.at[0], r_o.at[0], partner).wait_recv()
    rcopy(lst, lbuf.at[other], s_l.at[0], r_l.at[0], partner).wait_recv()
    place(other)
    out_v[...] = f_scr[...].astype(BF16)
    out_copy = pltpu.make_async_copy(out_v, out_hbm, out_sem.at[0])
    out_copy.start()
    lse = jnp.concatenate([lbuf[0, :2], lbuf[1, :2]], axis=0)
    hi = lse.astype(BF16)
    rest = lse - hi.astype(F32)
    mid = rest.astype(BF16)
    low = (rest - mid.astype(F32)).astype(BF16)
    lse_v[...] = nn(hi, perm[...]) + nn(mid, perm[...]) + nn(low, perm[...])
    lse_copy = pltpu.make_async_copy(lse_v, lse_hbm, out_sem.at[1])
    lse_copy.start()

    for cp in sends:
        cp.wait_send()
    for half in range(2):
        for dev in range(2):
            fwd_v(dev, half).wait_send()
            fwd_k(dev, half).wait_send()
    o_send.wait_send()
    l_send.wait_send()
    out_copy.wait()
    lse_copy.wait()


def solution(mesh):
    freq = (THETA ** (-(np.arange(64, dtype=np.float64) * 2.0) / D)).astype(np.float32)
    freq = np.broadcast_to(freq[:, None], (64, ROWS)).copy()
    any_spec = pl.BlockSpec(memory_space=pl.ANY)
    dma = pltpu.SemaphoreType.DMA
    vm = pltpu.VMEM

    def per_device(q_raw, k_raw, v_raw, positions, seq_ids, q_gain, k_gain):
        call = pl.pallas_call(
            kernel,
            out_shape=(jax.ShapeDtypeStruct((4 * ROWS, D), BF16), jax.ShapeDtypeStruct((4, ROWS), F32)),
            in_specs=[any_spec] * 8,
            out_specs=(any_spec, any_spec),
            scratch_shapes=[
                vm((4 * ROWS, D), BF16), vm((2 * ROWS, D), BF16), vm((2 * ROWS, D), BF16),
                vm((1, ROWS), jnp.int32), vm((1, ROWS), jnp.int32), vm((1, D), BF16), vm((1, D), BF16),
                vm((64, ROWS), F32),
                vm((4 * ROWS, D), F32), vm((2, 64, ROWS), F32), vm((ROWS, ROWS), BF16), vm((ROWS, ROWS), BF16),
                vm((4, 2, 2, HALF, D), BF16), vm((4, 2, 2, D, HALF), BF16),
                vm((2, 2, HALF, D), BF16), vm((2, 2, D, HALF), BF16),
                vm((2, 2, 2 * D, 2 * HALF), BF16), vm((2, D, 2 * HALF), BF16), vm((HALF, D), BF16),
                vm((2, 2, 1, 2 * HALF), F32), vm((2, 2, 1, 2 * HALF), F32), vm((2, 2, D, 2 * HALF), F32),
                vm((2, D, ROWS), BF16), vm((2, 2, D, ROWS), BF16), vm((8, ROWS), F32), vm((2, 8, ROWS), F32),
                vm((4 * ROWS, D), BF16), vm((4, ROWS), F32),
                dma((8,)), dma((2,)), dma((2, 2, 2)), dma((2, 2, 2)), dma((2, 2)), dma((2,)), dma((2, 2)), dma((2, 2)),
                dma((1,)), dma((1,)), dma((4, 2, 2)), dma((4, 2, 2)), dma((2,)), dma((1,)), dma((1,)),
            ],
            compiler_params=pltpu.CompilerParams(collective_id=0, has_side_effects=True, vmem_limit_bytes=40 * 1024 * 1024),
        )
        out, lse = call(q_raw.reshape(4 * ROWS, D), k_raw.reshape(2 * ROWS, D), v_raw.reshape(2 * ROWS, D),
                        positions.reshape(1, ROWS), seq_ids.reshape(1, ROWS), q_gain.reshape(1, D), k_gain.reshape(1, D),
                        jnp.asarray(freq))
        return out.reshape(ROWS, 4, D), lse.T

    return jax.shard_map(per_device, mesh=mesh, in_specs=(P("cp", "tp", None), P("cp", "tp", None), P("cp", "tp", None), P("cp"), P("cp"), P(), P()), out_specs=(P("cp", "tp", None), P("cp", "tp")), check_vma=False)
```

```python
import functools
import math

import jax
import jax.numpy as jnp
import numpy as np
from jax import lax
from jax.experimental import pallas as pl
from jax.experimental.pallas import tpu as pltpu
from jax.sharding import PartitionSpec as P

THETA = 1000000.0
EPS = 1e-6
NEG_BIG = -1e30
D = 128
HALF = 256
ROWS = 512
C_EXP = (D ** -0.5) * math.log2(math.e)
SCALE = D ** -0.5
F32 = jnp.float32
BF16 = jnp.bfloat16


def nt(a, b):
    return lax.dot_general(a, b, (((1,), (1,)), ((), ())), preferred_element_type=F32)


def nn(a, b):
    return lax.dot_general(a, b, (((1,), (0,)), ((), ())), preferred_element_type=F32)


def kernel(q_hbm, k_hbm, v_hbm, pos_hbm, seq_hbm, qg_hbm, kg_hbm, freq_hbm, out_ref, lse_out,
           q_in, k_in, v_in, pos_v, seq_v, qg_v, kg_v, freq_v, f_scr, cs_scr, perm, perm_t,
           kbuf, vbuf, kst, vst, qbuf, qst, kaug, m_scr, l_scr, acc, ost, obuf, lst, lbuf, pbuf,
           in_sem, s_kx, s_vx, s_p, s_q, s_fk, s_fv, s_o, s_l, r_k, r_v, r_q, r_o, r_l):
    me = lax.axis_index("cp")
    core = lax.rem(me, 2)
    chip = lax.div(me, 2)
    x = lax.rem(chip, 2)
    y = lax.div(chip, 2)
    xchip = chip + 1 - 2 * x
    ychip = chip + 2 - 4 * y
    other = 1 - core
    partner = 2 * chip + other

    def rcopy(src, dst, ssem, rsem, dev):
        return pltpu.make_async_remote_copy(src_ref=src, dst_ref=dst, send_sem=ssem, recv_sem=rsem,
                                            device_id={"cp": dev}, device_id_type=pl.DeviceIdType.MESH)

    barrier = pltpu.get_barrier_semaphore()
    peers = [partner, 2 * xchip, 2 * xchip + 1, 2 * ychip, 2 * ychip + 1]
    for peer in peers:
        pl.semaphore_signal(barrier, inc=1, device_id={"cp": peer}, device_id_type=pl.DeviceIdType.MESH)

    ins = [(v_hbm, v_in), (seq_hbm, seq_v), (pos_hbm, pos_v), (k_hbm, k_in), (kg_hbm, kg_v), (freq_hbm, freq_v),
           (q_hbm, q_in), (qg_hbm, qg_v)]
    in_copies = [pltpu.make_async_copy(src, dst, in_sem.at[n]) for n, (src, dst) in enumerate(ins)]
    for cp in in_copies:
        cp.start()

    in_copies[1].wait()
    seq = seq_v[...]
    row_id = lax.broadcasted_iota(jnp.int32, (8, ROWS), 1).astype(F32)
    sub_id = lax.broadcasted_iota(jnp.int32, (8, ROWS), 0)
    is_seq = jnp.broadcast_to(seq, (8, ROWS)) == sub_id
    seq_f = jnp.where(is_seq, 1.0, 0.0)
    cnt = jnp.sum(seq_f, axis=1, keepdims=True)
    start = jnp.min(jnp.where(is_seq, row_id, float(ROWS)), axis=1, keepdims=True)
    start_row = jnp.sum(seq_f * start, axis=0, keepdims=True)
    cnt_row = jnp.sum(seq_f * cnt, axis=0, keepdims=True)
    off = row_id[:1] - start_row
    late = off * 2.0 >= cnt_row
    dest = start_row * 0.5 + off + jnp.where(late, HALF - 0.5 * cnt_row, 0.0)
    dest_i = dest.astype(jnp.int32)
    for blk in range(4):
        rows = lax.broadcasted_iota(jnp.int32, (128, ROWS), 0) + blk * 128
        perm[pl.ds(blk * 128, 128), :] = jnp.where(rows == dest_i, 1.0, 0.0).astype(BF16)

    in_copies[0].wait()
    f_scr[pl.ds(0, 1024), :] = v_in[...].astype(F32)
    for h in range(2):
        vt = f_scr[pl.ds(h, ROWS, stride=2), :].T.astype(BF16)
        vc = nt(vt, perm[...]).astype(BF16)
        for half in range(2):
            vst[h, half] = vc[:, half * HALF:(half + 1) * HALF]
    for half in range(2):
        vbuf[0, half, core] = vst[core, half]
    pl.semaphore_wait(barrier, 5)

    sends = []

    def send_v(half):
        for h in range(2):
            for t, tchip in enumerate((xchip, ychip)):
                sends.append(rcopy(vst.at[h, half], vbuf.at[1 + t, half, core], s_vx.at[t, h, half],
                                   r_v.at[1 + t, core, half], 2 * tchip + h))
                sends[-1].start()

    def send_k(half):
        for h in range(2):
            for t, tchip in enumerate((xchip, ychip)):
                sends.append(rcopy(kst.at[h, half], kbuf.at[1 + t, half, core], s_kx.at[t, h, half],
                                   r_k.at[1 + t, core, half], 2 * tchip + h))
                sends[-1].start()

    send_v(0)
    for half in range(2):
        sends.append(rcopy(vst.at[other, half], vbuf.at[0, half, core], s_p.at[0, half], r_v.at[0, core, half], partner))
        sends[-1].start()

    in_copies[2].wait()
    in_copies[5].wait()
    angle = freq_v[...] * pos_v[...].astype(F32)
    cs_scr[0] = jnp.cos(angle)
    cs_scr[1] = jnp.sin(angle)

    def norm_rope(rows_f32, gain_v):
        xt = rows_f32.T
        inv = lax.rsqrt(jnp.mean(xt * xt, axis=0, keepdims=True) + EPS)
        gain = jnp.broadcast_to(gain_v[...].astype(F32), (128, D)).T
        gain = jnp.concatenate([gain] * 4, axis=1)
        n = (xt * inv * gain).astype(BF16).astype(F32)
        a, b = n[:64], n[64:]
        cos, sin = cs_scr[0], cs_scr[1]
        return jnp.concatenate([a * cos - b * sin, b * cos + a * sin], axis=0).astype(BF16)

    in_copies[3].wait()
    in_copies[4].wait()
    f_scr[pl.ds(0, 1024), :] = k_in[...].astype(F32)
    for h in range(2):
        kr = norm_rope(f_scr[pl.ds(h, ROWS, stride=2), :], kg_v)
        kc = nt(perm[...], kr).astype(BF16)
        for half in range(2):
            kst[h, half] = kc[half * HALF:(half + 1) * HALF, :]
    for half in range(2):
        kbuf[0, half, core] = kst[core, half]

    send_k(0)
    send_v(1)
    send_k(1)
    for half in range(2):
        sends.append(rcopy(kst.at[other, half], kbuf.at[0, half, core], s_p.at[1, half], r_k.at[0, core, half], partner))
        sends[-1].start()

    in_copies[6].wait()
    in_copies[7].wait()
    f_scr[...] = q_in[...].astype(F32)

    def q_head(h, store):
        qr = norm_rope(f_scr[pl.ds(h, ROWS, stride=4), :], qg_v)
        qc = nt(qr, perm[...]).astype(BF16)
        for half in range(2):
            store(half, qc[:, half * HALF:(half + 1) * HALF])

    for g in range(2):
        def store_other(half, val, g=g):
            qst[half, :, g * HALF:(g + 1) * HALF] = val
        q_head(2 * other + g, store_other)
    for half in range(2):
        sends.append(rcopy(qst.at[half], qbuf.at[half, 0, pl.ds(0, D), :], s_q.at[half], r_q.at[half], partner))
        sends[-1].start()
    for g in range(2):
        def store_own(half, val, g=g):
            qbuf[half, 1, pl.ds(0, D), g * HALF:(g + 1) * HALF] = val
        q_head(2 * core + g, store_own)

    lane_d = lax.broadcasted_iota(jnp.int32, (8, HALF), 1).astype(F32)
    in_run = (lane_d >= start * 0.5) & (lane_d < (start + cnt) * 0.5)
    one_hot = jnp.where(in_run, 1.0, 0.0)
    blocked = jnp.where(in_run, 0.0, NEG_BIG)
    blocked = jnp.where(lax.broadcasted_iota(jnp.int32, (8, HALF), 0) < 4, blocked, 0.0)
    pad = jnp.zeros((D - 8, HALF), F32)
    q_extra = jnp.concatenate([blocked, pad], axis=0).astype(BF16)
    for half in range(2):
        for dev in range(2):
            for g in range(2):
                qbuf[half, dev, pl.ds(D, D), g * HALF:(g + 1) * HALF] = q_extra
    kaug[...] = jnp.concatenate([one_hot, pad], axis=0).T.astype(BF16)

    dest_cols = jnp.broadcast_to(dest, (128, ROWS)).T.astype(jnp.int32)
    for blk in range(4):
        lanes = lax.broadcasted_iota(jnp.int32, (ROWS, 128), 1) + blk * 128
        perm_t[blk // 2, :, (blk % 2) * 128:(blk % 2 + 1) * 128] = jnp.where(lanes == dest_cols, 1.0, 0.0).astype(BF16)

    m_scr[...] = jnp.full(m_scr.shape, NEG_BIG, F32)
    l_scr[...] = jnp.zeros(l_scr.shape, F32)
    acc[...] = jnp.zeros(acc.shape, F32)

    def tile_parts(slot, khalf, qhalf, causal):
        keys = kbuf[slot, khalf].reshape(2 * HALF, D)
        ka = kaug[...]
        keys = jnp.concatenate([keys, jnp.concatenate([ka, ka], axis=0)], axis=1)
        v0 = vbuf[slot, khalf, 0]
        v1 = vbuf[slot, khalf, 1]
        chunks = [(dev, g) for dev in range(2) for g in range(2)]

        def scores(n):
            dev, g = chunks[n]
            s = nn(keys, qbuf[qhalf, dev, :, pl.ds(g * HALF, HALF)])
            if causal:
                abs_dev = core if dev == 1 else other
                krow = lax.broadcasted_iota(jnp.int32, (2 * HALF, HALF), 0)
                qcol = lax.broadcasted_iota(jnp.int32, (2 * HALF, HALF), 1)
                kord = krow + qhalf * jnp.where(krow < HALF, HALF, -HALF)
                qord = qcol + (abs_dev + qhalf * (1 - 2 * abs_dev)) * HALF
                s = jnp.where(kord <= qord, s, NEG_BIG)
            return s

        def soft(n, s):
            dev, g = chunks[n]
            cols = pl.ds(g * HALF, HALF)
            m_old = m_scr[qhalf, dev, :, cols]
            m_new = jnp.maximum(m_old, jnp.max(s, axis=0, keepdims=True))
            p = jnp.exp2((s - m_new) * C_EXP)
            alpha = jnp.exp2((m_old - m_new) * C_EXP)
            m_scr[qhalf, dev, :, cols] = m_new
            l_scr[qhalf, dev, :, cols] = l_scr[qhalf, dev, :, cols] * alpha + jnp.sum(p, axis=0, keepdims=True)
            return p.astype(BF16), alpha

        def out(n, pb, alpha):
            dev, g = chunks[n]
            cols = pl.ds(g * HALF, HALF)
            o = nn(v0, pb[:HALF]) + nn(v1, pb[HALF:])
            acc[qhalf, dev, :, cols] = acc[qhalf, dev, :, cols] * alpha + o

        return scores, soft, out

    def tile(slot, khalf, qhalf, causal):
        scores, soft, out = tile_parts(slot, khalf, qhalf, causal)
        s = scores(0)
        prev = None
        for n in range(4):
            nxt = scores(n + 1) if n < 3 else None
            pb, alpha = soft(n, s)
            if prev is not None:
                out(n - 1, *prev)
            prev = (pb, alpha)
            s = nxt
        out(3, *prev)

    def got_k(slot, dev, half):
        rcopy(kst.at[0, half], kbuf.at[slot, half, dev], s_kx.at[0, 0, half], r_k.at[slot, dev, half], partner).wait_recv()

    def got_v(slot, dev, half):
        rcopy(vst.at[0, half], vbuf.at[slot, half, dev], s_vx.at[0, 0, half], r_v.at[slot, dev, half], partner).wait_recv()

    for half in range(2):
        got_v(0, other, half)
        got_k(0, other, half)
        rcopy(qst.at[half], qbuf.at[half, 0, pl.ds(0, D), :], s_q.at[half], r_q.at[half], partner).wait_recv()

    def own_body(half, carry):
        tile(0, half, half, True)
        return carry

    lax.fori_loop(0, 2, own_body, 0)

    def fwd_v(dev, half):
        slot, to = (2, xchip) if dev == 0 else (1, ychip)
        return rcopy(vbuf.at[slot, half, dev], vbuf.at[3, half, dev], s_fv.at[dev, half], r_v.at[3, dev, half], 2 * to + core)

    def fwd_k(dev, half):
        slot, to = (2, xchip) if dev == 0 else (1, ychip)
        return rcopy(kbuf.at[slot, half, dev], kbuf.at[3, half, dev], s_fk.at[dev, half], r_k.at[3, dev, half], 2 * to + core)

    def body(idx, carry):
        @pl.when(idx == 1)
        def _():
            for dev in range(2):
                got_v(2 - dev, dev, 0)
                fwd_v(dev, 0).start()
            for dev in range(2):
                got_k(2 - dev, dev, 0)
                fwd_k(dev, 0).start()
            got_v(1, 0, 0)
            got_k(1, 0, 0)

        @pl.when(idx == 2)
        def _():
            got_v(2, 1, 0)
            got_k(2, 1, 0)

        @pl.when(idx == 3)
        def _():
            for dev in range(2):
                got_k(2 - dev, dev, 1)
                fwd_k(dev, 1).start()
            for dev in range(2):
                got_v(2 - dev, dev, 1)
                fwd_v(dev, 1).start()
            got_v(1, 0, 1)
            got_k(1, 0, 1)

        @pl.when(idx == 4)
        def _():
            got_v(2, 1, 1)
            got_k(2, 1, 1)

        @pl.when(idx == 5)
        def _():
            for dev in range(2):
                got_v(3, dev, 0)
                got_k(3, dev, 0)

        second = (idx // 3) * (1 - idx // 5)
        slot = idx - 2 * second - 2 * (idx // 5)
        late_needed = (1 - y) + (idx % 2) * (y - x)
        sel = second * late_needed
        tile(slot, sel, 1 - second + sel, False)
        return carry

    lax.fori_loop(0, 6, body, 0)

    done = y
    last = 1 - y

    def place(grp, half, first):
        for g in range(2):
            rows = pl.ds(2 * grp + g, ROWS, stride=4)
            val = nt(perm_t[half], obuf[grp, half, g])
            f_scr[rows, :] = val if first else f_scr[rows, :] + val

    def give(half, n):
        return rcopy(ost.at[half], obuf.at[core, half], s_o.at[n], r_o.at[n], partner)

    def take(half, n):
        rcopy(ost.at[half], obuf.at[other, half], s_o.at[n], r_o.at[n], partner).wait_recv()

    for g in range(2):
        cols = pl.ds(g * HALF, HALF)
        ost[done, g] = (acc[done, 0, :, cols] * (1.0 / l_scr[done, 0, :, cols])).astype(BF16)
    give(done, 0).start()
    for g in range(2):
        cols = pl.ds(g * HALF, HALF)
        obuf[core, done, g] = (acc[done, 1, :, cols] * (1.0 / l_scr[done, 1, :, cols])).astype(BF16)
    place(core, done, True)

    for dev in range(2):
        got_k(3, dev, 1)
    scores, soft, _ = tile_parts(3, last, last, False)
    s = scores(0)
    for n in range(4):
        nxt = scores(n + 1) if n < 3 else None
        pb, alpha = soft(n, s)
        pbuf[n] = pb
        cols = pl.ds((n % 2) * HALF, HALF)
        acc[last, n // 2, :, cols] = acc[last, n // 2, :, cols] * alpha
        s = nxt
    for dev in range(2):
        for half in range(2):
            for g in range(2):
                cols = pl.ds(g * HALF, HALF)
                val = m_scr[half, dev, :, cols] * SCALE + jnp.log(l_scr[half, dev, :, cols])
                if dev == 0:
                    lst[pl.ds(g, 1), half * HALF:(half + 1) * HALF] = val
                else:
                    lbuf[core, pl.ds(g, 1), half * HALF:(half + 1) * HALF] = val
        if dev == 0:
            l_send = rcopy(lst, lbuf.at[core], s_l.at[0], r_l.at[0], partner)
            l_send.start()
    take(done, 0)
    place(other, done, True)

    for dev in range(2):
        got_v(3, dev, 1)
    for n in range(4):
        cols = pl.ds((n % 2) * HALF, HALF)
        dev, g = n // 2, n % 2
        o = nn(vbuf[3, last, 0], pbuf[n, :HALF, :]) + nn(vbuf[3, last, 1], pbuf[n, HALF:, :])
        o = ((acc[last, dev, :, cols] + o) * (1.0 / l_scr[last, dev, :, cols])).astype(BF16)
        if dev == 0:
            ost[last, g] = o
        else:
            obuf[core, last, g] = o
        if n == 1:
            give(last, 1).start()
    place(core, last, False)
    rcopy(lst, lbuf.at[other], s_l.at[0], r_l.at[0], partner).wait_recv()
    lse = jnp.concatenate([lbuf[0, :2], lbuf[1, :2]], axis=0)
    hi = lse.astype(BF16).astype(F32)
    rest = lse - hi
    mid = rest.astype(BF16).astype(F32)
    pieces = jnp.concatenate([hi, mid, rest - mid, jnp.zeros((4, ROWS), F32)], axis=0).astype(BF16)
    pieces = nn(pieces, perm[...])
    lse_out[...] = pieces[0:4] + pieces[4:8] + pieces[8:12]
    take(last, 1)
    place(other, last, False)
    out_ref[...] = f_scr[...].astype(BF16)

    for cp in sends:
        cp.wait_send()
    for half in range(2):
        for dev in range(2):
            fwd_v(dev, half).wait_send()
            fwd_k(dev, half).wait_send()
    give(done, 0).wait_send()
    give(last, 1).wait_send()
    l_send.wait_send()


def write_out(o_ref, l_ref, o_hbm, l_hbm, sem):
    copies = [pltpu.make_async_copy(o_ref, o_hbm, sem.at[0]), pltpu.make_async_copy(l_ref, l_hbm, sem.at[1])]
    for cp in copies:
        cp.start()
    for cp in copies:
        cp.wait()


def solution(mesh):
    freq = (THETA ** (-(np.arange(64, dtype=np.float64) * 2.0) / D)).astype(np.float32)
    freq = np.broadcast_to(freq[:, None], (64, ROWS)).copy()
    any_spec = pl.BlockSpec(memory_space=pl.ANY)
    dma = pltpu.SemaphoreType.DMA
    vm = pltpu.VMEM

    def per_device(q_raw, k_raw, v_raw, positions, seq_ids, q_gain, k_gain):
        call = pl.pallas_call(
            kernel,
            out_shape=(jax.ShapeDtypeStruct((4 * ROWS, D), BF16), jax.ShapeDtypeStruct((4, ROWS), F32)),
            in_specs=[any_spec] * 8,
            out_specs=(pl.BlockSpec(memory_space=pltpu.VMEM), pl.BlockSpec(memory_space=pltpu.VMEM)),
            scratch_shapes=[
                vm((4 * ROWS, D), BF16), vm((2 * ROWS, D), BF16), vm((2 * ROWS, D), BF16),
                vm((1, ROWS), jnp.int32), vm((1, ROWS), jnp.int32), vm((1, D), BF16), vm((1, D), BF16),
                vm((64, ROWS), F32),
                vm((4 * ROWS, D), F32), vm((2, 64, ROWS), F32), vm((ROWS, ROWS), BF16), vm((2, ROWS, HALF), BF16),
                vm((4, 2, 2, HALF, D), BF16), vm((4, 2, 2, D, HALF), BF16),
                vm((2, 2, HALF, D), BF16), vm((2, 2, D, HALF), BF16),
                vm((2, 2, 2 * D, 2 * HALF), BF16), vm((2, D, 2 * HALF), BF16), vm((HALF, D), BF16),
                vm((2, 2, 1, 2 * HALF), F32), vm((2, 2, 1, 2 * HALF), F32), vm((2, 2, D, 2 * HALF), F32),
                vm((2, 2, D, HALF), BF16), vm((2, 2, 2, D, HALF), BF16), vm((8, ROWS), F32), vm((2, 8, ROWS), F32),
                vm((4, 2 * HALF, HALF), BF16),
                dma((8,)), dma((2, 2, 2)), dma((2, 2, 2)), dma((2, 2)), dma((2,)), dma((2, 2)), dma((2, 2)),
                dma((2,)), dma((1,)), dma((4, 2, 2)), dma((4, 2, 2)), dma((2,)), dma((2,)), dma((1,)),
            ],
            compiler_params=pltpu.CompilerParams(collective_id=0, has_side_effects=True, vmem_limit_bytes=40000 * 1024),
        )
        args = (q_raw.reshape(4 * ROWS, D), k_raw.reshape(2 * ROWS, D), v_raw.reshape(2 * ROWS, D),
                positions.reshape(1, ROWS), seq_ids.reshape(1, ROWS), q_gain.reshape(1, D), k_gain.reshape(1, D),
                jnp.asarray(freq))
        args = [pltpu.with_memory_space_constraint(a, pltpu.HBM) for a in args]
        out, lse = call(*args)
        out, lse = pl.pallas_call(
            write_out,
            out_shape=(jax.ShapeDtypeStruct((4 * ROWS, D), BF16), jax.ShapeDtypeStruct((4, ROWS), F32)),
            in_specs=[pl.BlockSpec(memory_space=pltpu.VMEM)] * 2,
            out_specs=(pl.BlockSpec(memory_space=pltpu.HBM), pl.BlockSpec(memory_space=pltpu.HBM)),
            scratch_shapes=[dma((2,))],
            compiler_params=pltpu.CompilerParams(vmem_limit_bytes=1024*1024),
        )(out, lse)
        return out.reshape(ROWS, 4, D), lse.T

    return jax.shard_map(per_device, mesh=mesh, in_specs=(P("cp", "tp", None), P("cp", "tp", None), P("cp", "tp", None), P("cp"), P("cp"), P(), P()), out_specs=(P("cp", "tp", None), P("cp", "tp")), check_vma=False)
```

```python
import functools
import math

import jax
import jax.numpy as jnp
import numpy as np
from jax import lax
from jax.experimental import pallas as pl
from jax.experimental.pallas import tpu as pltpu
from jax.sharding import PartitionSpec as P

THETA = 1000000.0
EPS = 1e-6
NEG_BIG = -1e30
D = 128
HALF = 256
ROWS = 512
C_EXP = (D ** -0.5) * math.log2(math.e)
SCALE = D ** -0.5
F32 = jnp.float32
BF16 = jnp.bfloat16


def nt(a, b):
    return lax.dot_general(a, b, (((1,), (1,)), ((), ())), preferred_element_type=F32)


def nn(a, b):
    return lax.dot_general(a, b, (((1,), (0,)), ((), ())), preferred_element_type=F32)


def kernel(q_hbm, k_hbm, v_hbm, pos_hbm, seq_hbm, qg_hbm, kg_hbm, freq_hbm, out_ref, lse_out,
           q_in, k_in, v_in, pos_v, seq_v, qg_v, kg_v, freq_v, f_scr, cs_scr, perm, perm_t,
           kbuf, vbuf, vraw, kst, vst, qbuf, qst, kaug, m_scr, l_scr, acc, ost, obuf, lst, lbuf, pbuf,
           in_sem, ready, s_raw, r_raw, s_kx, s_v, s_p, s_q, s_fk, s_fv, s_o, s_l, r_k, r_v, r_q, r_o, r_l):
    me = lax.axis_index("cp")
    core = lax.rem(me, 2)
    chip = lax.div(me, 2)
    x = lax.rem(chip, 2)
    y = lax.div(chip, 2)
    xchip = chip + 1 - 2 * x
    ychip = chip + 2 - 4 * y
    other = 1 - core
    partner = 2 * chip + other

    def rcopy(src, dst, ssem, rsem, dev):
        return pltpu.make_async_remote_copy(src_ref=src, dst_ref=dst, send_sem=ssem, recv_sem=rsem,
                                            device_id={"cp": dev}, device_id_type=pl.DeviceIdType.MESH)

    barrier = pltpu.get_barrier_semaphore()
    for peer in (2 * xchip, 2 * ychip + 1, partner):
        pl.semaphore_signal(barrier, inc=1, device_id={"cp": peer}, device_id_type=pl.DeviceIdType.MESH)

    ins = [(v_hbm, v_in), (seq_hbm, seq_v), (pos_hbm, pos_v), (k_hbm, k_in), (kg_hbm, kg_v), (freq_hbm, freq_v),
           (q_hbm, q_in), (qg_hbm, qg_v)]
    in_copies = [pltpu.make_async_copy(src, dst, in_sem.at[n]) for n, (src, dst) in enumerate(ins)]
    for n in (1, 2, 5, 3, 4, 0, 6, 7):
        in_copies[n].start()

    pl.semaphore_wait(barrier, 3)
    pl.semaphore_signal(ready, inc=1, device_id={"cp": partner}, device_id_type=pl.DeviceIdType.MESH)

    def raw_v(t):
        tchip = xchip + t * (ychip - xchip)
        return rcopy(v_hbm, vraw.at[t], s_raw.at[t], r_raw.at[t], 2 * tchip + core)

    raw_v(core).start()
    pl.semaphore_wait(ready, 1)
    raw_v(other).start()

    in_copies[1].wait()
    seq = seq_v[...]
    row_id = lax.broadcasted_iota(jnp.int32, (8, ROWS), 1).astype(F32)
    sub_id = lax.broadcasted_iota(jnp.int32, (8, ROWS), 0)
    is_seq = jnp.broadcast_to(seq, (8, ROWS)) == sub_id
    seq_f = jnp.where(is_seq, 1.0, 0.0)
    cnt = jnp.sum(seq_f, axis=1, keepdims=True)
    start = jnp.min(jnp.where(is_seq, row_id, float(ROWS)), axis=1, keepdims=True)
    start_row = jnp.sum(seq_f * start, axis=0, keepdims=True)
    cnt_row = jnp.sum(seq_f * cnt, axis=0, keepdims=True)
    off = row_id[:1] - start_row
    late = off * 2.0 >= cnt_row
    dest = start_row * 0.5 + off + jnp.where(late, HALF - 0.5 * cnt_row, 0.0)
    dest_i = dest.astype(jnp.int32)
    for blk in range(4):
        rows = lax.broadcasted_iota(jnp.int32, (128, ROWS), 0) + blk * 128
        perm[pl.ds(blk * 128, 128), :] = jnp.where(rows == dest_i, 1.0, 0.0).astype(BF16)

    sends = []

    def send_k(half):
        for h in range(2):
            for t, tchip in enumerate((xchip, ychip)):
                sends.append(rcopy(kst.at[h, half], kbuf.at[1 + t, half, core], s_kx.at[t, h, half],
                                   r_k.at[1 + t, core, half], 2 * tchip + h))
                sends[-1].start()

    def v_share(slot, half):
        return rcopy(vst.at[slot, half], vbuf.at[slot, half, core], s_v.at[slot, half], r_v.at[slot, core, half], partner)

    def split_v(src, slot):
        f_scr[pl.ds(0, 2 * ROWS), :] = src[...].astype(F32)
        for mine in range(2):
            h = core if mine else other
            vt = f_scr[pl.ds(h, ROWS, stride=2), :].T.astype(BF16)
            vc = nt(vt, perm[...]).astype(BF16)
            for half in range(2):
                part = vc[:, half * HALF:(half + 1) * HALF]
                if mine:
                    vbuf[slot, half, core] = part
                else:
                    vst[slot, half] = part
        for half in range(2):
            v_share(slot, half).start()

    in_copies[2].wait()
    in_copies[5].wait()
    angle = freq_v[...] * pos_v[...].astype(F32)
    cs_scr[0] = jnp.cos(angle)
    cs_scr[1] = jnp.sin(angle)

    def norm_rope(rows_f32, gain_v):
        xt = rows_f32.T
        inv = lax.rsqrt(jnp.mean(xt * xt, axis=0, keepdims=True) + EPS)
        gain = jnp.broadcast_to(gain_v[...].astype(F32), (128, D)).T
        gain = jnp.concatenate([gain] * 4, axis=1)
        n = (xt * inv * gain).astype(BF16).astype(F32)
        a, b = n[:64], n[64:]
        cos, sin = cs_scr[0], cs_scr[1]
        return jnp.concatenate([a * cos - b * sin, b * cos + a * sin], axis=0).astype(BF16)

    in_copies[3].wait()
    in_copies[4].wait()
    f_scr[pl.ds(0, 1024), :] = k_in[...].astype(F32)
    for h in range(2):
        kr = norm_rope(f_scr[pl.ds(h, ROWS, stride=2), :], kg_v)
        kc = nt(perm[...], kr).astype(BF16)
        for half in range(2):
            kst[h, half] = kc[half * HALF:(half + 1) * HALF, :]
    for half in range(2):
        kbuf[0, half, core] = kst[core, half]

    send_k(0)
    send_k(1)
    for half in range(2):
        sends.append(rcopy(kst.at[other, half], kbuf.at[0, half, core], s_p.at[half], r_k.at[0, core, half], partner))
        sends[-1].start()

    in_copies[0].wait()
    split_v(v_in, 0)

    in_copies[6].wait()
    in_copies[7].wait()
    f_scr[...] = q_in[...].astype(F32)

    def q_head(h, store):
        qr = norm_rope(f_scr[pl.ds(h, ROWS, stride=4), :], qg_v)
        qc = nt(qr, perm[...]).astype(BF16)
        for half in range(2):
            store(half, qc[:, half * HALF:(half + 1) * HALF])

    for g in range(2):
        def store_other(half, val, g=g):
            qst[half, :, g * HALF:(g + 1) * HALF] = val
        q_head(2 * other + g, store_other)
    for half in range(2):
        sends.append(rcopy(qst.at[half], qbuf.at[half, 0, pl.ds(0, D), :], s_q.at[half], r_q.at[half], partner))
        sends[-1].start()
    for g in range(2):
        def store_own(half, val, g=g):
            qbuf[half, 1, pl.ds(0, D), g * HALF:(g + 1) * HALF] = val
        q_head(2 * core + g, store_own)

    lane_d = lax.broadcasted_iota(jnp.int32, (8, HALF), 1).astype(F32)
    in_run = (lane_d >= start * 0.5) & (lane_d < (start + cnt) * 0.5)
    one_hot = jnp.where(in_run, 1.0, 0.0)
    blocked = jnp.where(in_run, 0.0, NEG_BIG)
    blocked = jnp.where(lax.broadcasted_iota(jnp.int32, (8, HALF), 0) < 4, blocked, 0.0)
    pad = jnp.zeros((D - 8, HALF), F32)
    q_extra = jnp.concatenate([blocked, pad], axis=0).astype(BF16)
    for half in range(2):
        for dev in range(2):
            for g in range(2):
                qbuf[half, dev, pl.ds(D, D), g * HALF:(g + 1) * HALF] = q_extra
    kaug[...] = jnp.concatenate([one_hot, pad], axis=0).T.astype(BF16)

    dest_cols = jnp.broadcast_to(dest, (128, ROWS)).T.astype(jnp.int32)
    for blk in range(4):
        lanes = lax.broadcasted_iota(jnp.int32, (ROWS, 128), 1) + blk * 128
        perm_t[blk // 2, :, (blk % 2) * 128:(blk % 2 + 1) * 128] = jnp.where(lanes == dest_cols, 1.0, 0.0).astype(BF16)

    m_scr[...] = jnp.full(m_scr.shape, NEG_BIG, F32)
    l_scr[...] = jnp.zeros(l_scr.shape, F32)
    acc[...] = jnp.zeros(acc.shape, F32)

    def tile_parts(slot, khalf, qhalf, causal):
        keys = kbuf[slot, khalf].reshape(2 * HALF, D)
        ka = kaug[...]
        keys = jnp.concatenate([keys, jnp.concatenate([ka, ka], axis=0)], axis=1)
        v0 = vbuf[slot, khalf, 0]
        v1 = vbuf[slot, khalf, 1]
        chunks = [(dev, g) for dev in range(2) for g in range(2)]

        def scores(n):
            dev, g = chunks[n]
            s = nn(keys, qbuf[qhalf, dev, :, pl.ds(g * HALF, HALF)])
            if causal:
                abs_dev = core if dev == 1 else other
                krow = lax.broadcasted_iota(jnp.int32, (2 * HALF, HALF), 0)
                qcol = lax.broadcasted_iota(jnp.int32, (2 * HALF, HALF), 1)
                kord = krow + qhalf * jnp.where(krow < HALF, HALF, -HALF)
                qord = qcol + (abs_dev + qhalf * (1 - 2 * abs_dev)) * HALF
                s = jnp.where(kord <= qord, s, NEG_BIG)
            return s

        def soft(n, s):
            dev, g = chunks[n]
            cols = pl.ds(g * HALF, HALF)
            m_old = m_scr[qhalf, dev, :, cols]
            m_new = jnp.maximum(m_old, jnp.max(s, axis=0, keepdims=True))
            p = jnp.exp2((s - m_new) * C_EXP)
            alpha = jnp.exp2((m_old - m_new) * C_EXP)
            m_scr[qhalf, dev, :, cols] = m_new
            l_scr[qhalf, dev, :, cols] = l_scr[qhalf, dev, :, cols] * alpha + jnp.sum(p, axis=0, keepdims=True)
            return p.astype(BF16), alpha

        def out(n, pb, alpha):
            dev, g = chunks[n]
            cols = pl.ds(g * HALF, HALF)
            o = nn(v0, pb[:HALF]) + nn(v1, pb[HALF:])
            acc[qhalf, dev, :, cols] = acc[qhalf, dev, :, cols] * alpha + o

        return scores, soft, out

    def tile(slot, khalf, qhalf, causal):
        scores, soft, out = tile_parts(slot, khalf, qhalf, causal)
        s = scores(0)
        prev = None
        for n in range(4):
            nxt = scores(n + 1) if n < 3 else None
            pb, alpha = soft(n, s)
            if prev is not None:
                out(n - 1, *prev)
            prev = (pb, alpha)
            s = nxt
        out(3, *prev)

    def got_k(slot, dev, half):
        rcopy(kst.at[0, half], kbuf.at[slot, half, dev], s_kx.at[0, 0, half], r_k.at[slot, dev, half], partner).wait_recv()

    def got_v(slot, dev, half):
        rcopy(vst.at[0, half], vbuf.at[slot, half, dev], s_v.at[0, half], r_v.at[slot, dev, half], partner).wait_recv()

    for half in range(2):
        got_v(0, other, half)
        got_k(0, other, half)
        rcopy(qst.at[half], qbuf.at[half, 0, pl.ds(0, D), :], s_q.at[half], r_q.at[half], partner).wait_recv()

    def own_body(half, carry):
        tile(0, half, half, True)
        return carry

    lax.fori_loop(0, 2, own_body, 0)

    def fwd_v(dev, half):
        slot, to = (2, xchip) if dev == 0 else (1, ychip)
        return rcopy(vbuf.at[slot, half, dev], vbuf.at[3, half, dev], s_fv.at[dev, half], r_v.at[3, dev, half], 2 * to + core)

    def fwd_k(dev, half):
        slot, to = (2, xchip) if dev == 0 else (1, ychip)
        return rcopy(kbuf.at[slot, half, dev], kbuf.at[3, half, dev], s_fk.at[dev, half], r_k.at[3, dev, half], 2 * to + core)

    def body(idx, carry):
        @pl.when(idx == 1)
        def _():
            for t in range(2):
                raw_v(t).wait_recv()
                split_v(vraw.at[t], 1 + t)
            for half in range(2):
                for t in range(2):
                    got_v(1 + t, other, half)
            for dev in range(2):
                fwd_v(dev, 0).start()
            for dev in range(2):
                got_k(2 - dev, dev, 0)
                fwd_k(dev, 0).start()
            got_k(1, 0, 0)

        @pl.when(idx == 2)
        def _():
            got_k(2, 1, 0)

        @pl.when(idx == 3)
        def _():
            for dev in range(2):
                got_k(2 - dev, dev, 1)
                fwd_k(dev, 1).start()
            for dev in range(2):
                fwd_v(dev, 1).start()
            got_k(1, 0, 1)

        @pl.when(idx == 4)
        def _():
            got_k(2, 1, 1)

        @pl.when(idx == 5)
        def _():
            for dev in range(2):
                got_v(3, dev, 0)
                got_k(3, dev, 0)

        second = (idx // 3) * (1 - idx // 5)
        slot = idx - 2 * second - 2 * (idx // 5)
        late_needed = (1 - y) + (idx % 2) * (y - x)
        sel = second * late_needed
        tile(slot, sel, 1 - second + sel, False)
        return carry

    lax.fori_loop(0, 6, body, 0)

    done = y
    last = 1 - y

    def place(grp, half, first):
        for g in range(2):
            rows = pl.ds(2 * grp + g, ROWS, stride=4)
            val = nt(perm_t[half], obuf[grp, half, g])
            f_scr[rows, :] = val if first else f_scr[rows, :] + val

    def give(half, n):
        return rcopy(ost.at[half], obuf.at[core, half], s_o.at[n], r_o.at[n], partner)

    def take(half, n):
        rcopy(ost.at[half], obuf.at[other, half], s_o.at[n], r_o.at[n], partner).wait_recv()

    for g in range(2):
        cols = pl.ds(g * HALF, HALF)
        ost[done, g] = (acc[done, 0, :, cols] * (1.0 / l_scr[done, 0, :, cols])).astype(BF16)
    give(done, 0).start()
    for g in range(2):
        cols = pl.ds(g * HALF, HALF)
        obuf[core, done, g] = (acc[done, 1, :, cols] * (1.0 / l_scr[done, 1, :, cols])).astype(BF16)
    place(core, done, True)

    for dev in range(2):
        got_k(3, dev, 1)
    scores, soft, _ = tile_parts(3, last, last, False)
    s = scores(0)
    for n in range(4):
        nxt = scores(n + 1) if n < 3 else None
        pb, alpha = soft(n, s)
        pbuf[n] = pb
        cols = pl.ds((n % 2) * HALF, HALF)
        acc[last, n // 2, :, cols] = acc[last, n // 2, :, cols] * alpha
        s = nxt
    for dev in range(2):
        for half in range(2):
            for g in range(2):
                cols = pl.ds(g * HALF, HALF)
                val = m_scr[half, dev, :, cols] * SCALE + jnp.log(l_scr[half, dev, :, cols])
                if dev == 0:
                    lst[pl.ds(g, 1), half * HALF:(half + 1) * HALF] = val
                else:
                    lbuf[core, pl.ds(g, 1), half * HALF:(half + 1) * HALF] = val
        if dev == 0:
            l_send = rcopy(lst, lbuf.at[core], s_l.at[0], r_l.at[0], partner)
            l_send.start()
    take(done, 0)
    place(other, done, True)

    for dev in range(2):
        got_v(3, dev, 1)
    for n in range(4):
        cols = pl.ds((n % 2) * HALF, HALF)
        dev, g = n // 2, n % 2
        o = nn(vbuf[3, last, 0], pbuf[n, :HALF, :]) + nn(vbuf[3, last, 1], pbuf[n, HALF:, :])
        o = ((acc[last, dev, :, cols] + o) * (1.0 / l_scr[last, dev, :, cols])).astype(BF16)
        if dev == 0:
            ost[last, g] = o
        else:
            obuf[core, last, g] = o
        if n == 1:
            give(last, 1).start()
    place(core, last, False)
    rcopy(lst, lbuf.at[other], s_l.at[0], r_l.at[0], partner).wait_recv()
    lse = jnp.concatenate([lbuf[0, :2], lbuf[1, :2]], axis=0)
    hi = lse.astype(BF16).astype(F32)
    rest = lse - hi
    mid = rest.astype(BF16).astype(F32)
    pieces = jnp.concatenate([hi, mid, rest - mid, jnp.zeros((4, ROWS), F32)], axis=0).astype(BF16)
    pieces = nn(pieces, perm[...])
    lse_out[...] = pieces[0:4] + pieces[4:8] + pieces[8:12]
    take(last, 1)
    place(other, last, False)
    out_ref[...] = f_scr[...].astype(BF16)

    for cp in sends:
        cp.wait_send()
    for t in range(2):
        raw_v(t).wait_send()
    for slot in range(3):
        for half in range(2):
            v_share(slot, half).wait_send()
    for half in range(2):
        for dev in range(2):
            fwd_v(dev, half).wait_send()
            fwd_k(dev, half).wait_send()
    give(done, 0).wait_send()
    give(last, 1).wait_send()
    l_send.wait_send()


def write_out(o_ref, l_ref, o_hbm, l_hbm, sem):
    copies = [pltpu.make_async_copy(o_ref, o_hbm, sem.at[0]), pltpu.make_async_copy(l_ref, l_hbm, sem.at[1])]
    for cp in copies:
        cp.start()
    for cp in copies:
        cp.wait()


def solution(mesh):
    freq = (THETA ** (-(np.arange(64, dtype=np.float64) * 2.0) / D)).astype(np.float32)
    freq = np.broadcast_to(freq[:, None], (64, ROWS)).copy()
    any_spec = pl.BlockSpec(memory_space=pl.ANY)
    dma = pltpu.SemaphoreType.DMA
    vm = pltpu.VMEM

    def per_device(q_raw, k_raw, v_raw, positions, seq_ids, q_gain, k_gain):
        call = pl.pallas_call(
            kernel,
            out_shape=(jax.ShapeDtypeStruct((4 * ROWS, D), BF16), jax.ShapeDtypeStruct((4, ROWS), F32)),
            in_specs=[any_spec] * 8,
            out_specs=(pl.BlockSpec(memory_space=pltpu.VMEM), pl.BlockSpec(memory_space=pltpu.VMEM)),
            scratch_shapes=[
                vm((4 * ROWS, D), BF16), vm((2 * ROWS, D), BF16), vm((2 * ROWS, D), BF16),
                vm((1, ROWS), jnp.int32), vm((1, ROWS), jnp.int32), vm((1, D), BF16), vm((1, D), BF16),
                vm((64, ROWS), F32),
                vm((4 * ROWS, D), F32), vm((2, 64, ROWS), F32), vm((ROWS, ROWS), BF16), vm((2, ROWS, HALF), BF16),
                vm((4, 2, 2, HALF, D), BF16), vm((4, 2, 2, D, HALF), BF16),
                vm((2, 2 * ROWS, D), BF16), vm((2, 2, HALF, D), BF16), vm((3, 2, D, HALF), BF16),
                vm((2, 2, 2 * D, 2 * HALF), BF16), vm((2, D, 2 * HALF), BF16), vm((HALF, D), BF16),
                vm((2, 2, 1, 2 * HALF), F32), vm((2, 2, 1, 2 * HALF), F32), vm((2, 2, D, 2 * HALF), F32),
                vm((2, 2, D, HALF), BF16), vm((2, 2, 2, D, HALF), BF16), vm((8, ROWS), F32), vm((2, 8, ROWS), F32),
                vm((4, 2 * HALF, HALF), BF16),
                dma((8,)), pltpu.SemaphoreType.REGULAR, dma((2,)), dma((2,)), dma((2, 2, 2)), dma((3, 2)), dma((2,)), dma((2,)), dma((2, 2)), dma((2, 2)),
                dma((2,)), dma((1,)), dma((4, 2, 2)), dma((4, 2, 2)), dma((2,)), dma((2,)), dma((1,)),
            ],
            compiler_params=pltpu.CompilerParams(collective_id=0, has_side_effects=True, vmem_limit_bytes=40000 * 1024),
        )
        args = (q_raw.reshape(4 * ROWS, D), k_raw.reshape(2 * ROWS, D), v_raw.reshape(2 * ROWS, D),
                positions.reshape(1, ROWS), seq_ids.reshape(1, ROWS), q_gain.reshape(1, D), k_gain.reshape(1, D),
                jnp.asarray(freq))
        args = [pltpu.with_memory_space_constraint(a, pltpu.HBM) for a in args]
        out, lse = call(*args)
        out, lse = pl.pallas_call(
            write_out,
            out_shape=(jax.ShapeDtypeStruct((4 * ROWS, D), BF16), jax.ShapeDtypeStruct((4, ROWS), F32)),
            in_specs=[pl.BlockSpec(memory_space=pltpu.VMEM)] * 2,
            out_specs=(pl.BlockSpec(memory_space=pltpu.HBM), pl.BlockSpec(memory_space=pltpu.HBM)),
            scratch_shapes=[dma((2,))],
            compiler_params=pltpu.CompilerParams(vmem_limit_bytes=1024*1024),
        )(out, lse)
        return out.reshape(ROWS, 4, D), lse.T

    return jax.shard_map(per_device, mesh=mesh, in_specs=(P("cp", "tp", None), P("cp", "tp", None), P("cp", "tp", None), P("cp"), P("cp"), P(), P()), out_specs=(P("cp", "tp", None), P("cp", "tp")), check_vma=False)
```

```python
import functools
import math

import jax
import jax.numpy as jnp
import numpy as np
from jax import lax
from jax.experimental import pallas as pl
from jax.experimental.pallas import tpu as pltpu
from jax.sharding import PartitionSpec as P

THETA = 1000000.0
EPS = 1e-6
NEG_BIG = -1e30
D = 128
HALF = 256
ROWS = 512
C_EXP = (D ** -0.5) * math.log2(math.e)
SCALE = D ** -0.5
F32 = jnp.float32
BF16 = jnp.bfloat16


def nt(a, b):
    return lax.dot_general(a, b, (((1,), (1,)), ((), ())), preferred_element_type=F32)


def nn(a, b):
    return lax.dot_general(a, b, (((1,), (0,)), ((), ())), preferred_element_type=F32)


def kernel(q_hbm, k_hbm, v_hbm, pos_hbm, seq_hbm, qg_hbm, kg_hbm, freq_hbm, out_ref, lse_out,
           q_in, k_in, v_in, pos_v, seq_v, qg_v, kg_v, freq_v, f_scr, cs_scr, perm, perm_t,
           kbuf, vbuf, vraw, kst, vst, qbuf, qst, kaug, m_scr, l_scr, acc, ost, obuf, lst, lbuf, pbuf,
           in_sem, ready, s_raw, r_raw, r_own, r_share, r_k, r_far, r_o, r_l):
    me = lax.axis_index("cp")
    core = lax.rem(me, 2)
    chip = lax.div(me, 2)
    x = lax.rem(chip, 2)
    y = lax.div(chip, 2)
    xchip = chip + 1 - 2 * x
    ychip = chip + 2 - 4 * y
    other = 1 - core
    partner = 2 * chip + other

    def rcopy(src, dst, ssem, rsem, dev):
        return pltpu.make_async_remote_copy(src_ref=src, dst_ref=dst, send_sem=ssem, recv_sem=rsem,
                                            device_id={"cp": dev}, device_id_type=pl.DeviceIdType.MESH)

    s_k, s_own, s_share, s_fwd, s_o, s_l = (in_sem.at[n] for n in (1, 2, 3, 4, 5, 0))

    def sized(kib):
        return kbuf.at[pl.ds(0, kib // 256)] if kib >= 256 else kbuf.at[0, pl.ds(0, kib // 128)]

    def sent(sem, kib):
        rcopy(sized(kib), sized(kib), sem, r_l.at[0], partner).wait_send()

    def arrived(sem, kib):
        rcopy(sized(kib), sized(kib), s_l, sem, partner).wait_recv()

    barrier = pltpu.get_barrier_semaphore()
    for peer in (2 * xchip, 2 * ychip + 1, partner):
        pl.semaphore_signal(barrier, inc=1, device_id={"cp": peer}, device_id_type=pl.DeviceIdType.MESH)

    ins = [(v_hbm, v_in), (seq_hbm, seq_v), (pos_hbm, pos_v), (k_hbm, k_in), (kg_hbm, kg_v), (freq_hbm, freq_v),
           (q_hbm, q_in), (qg_hbm, qg_v)]
    in_copies = [pltpu.make_async_copy(src, dst, in_sem.at[n]) for n, (src, dst) in enumerate(ins)]
    for n in (1, 2, 5, 3, 4, 0, 6, 7):
        in_copies[n].start()

    pl.semaphore_wait(barrier, 3)
    pl.semaphore_signal(ready, inc=1, device_id={"cp": partner}, device_id_type=pl.DeviceIdType.MESH)

    def raw_v(t):
        tchip = xchip + t * (ychip - xchip)
        return rcopy(v_hbm, vraw.at[t], s_raw.at[0], r_raw.at[t], 2 * tchip + core)

    raw_v(core).start()
    pl.semaphore_wait(ready, 1)
    raw_v(other).start()

    in_copies[1].wait()
    seq = seq_v[...]
    row_id = lax.broadcasted_iota(jnp.int32, (8, ROWS), 1).astype(F32)
    sub_id = lax.broadcasted_iota(jnp.int32, (8, ROWS), 0)
    is_seq = jnp.broadcast_to(seq, (8, ROWS)) == sub_id
    seq_f = jnp.where(is_seq, 1.0, 0.0)
    cnt = jnp.sum(seq_f, axis=1, keepdims=True)
    start = jnp.min(jnp.where(is_seq, row_id, float(ROWS)), axis=1, keepdims=True)
    start_row = jnp.sum(seq_f * start, axis=0, keepdims=True)
    cnt_row = jnp.sum(seq_f * cnt, axis=0, keepdims=True)
    off = row_id[:1] - start_row
    late = off * 2.0 >= cnt_row
    dest = start_row * 0.5 + off + jnp.where(late, HALF - 0.5 * cnt_row, 0.0)
    dest_i = dest.astype(jnp.int32)
    for blk in range(4):
        rows = lax.broadcasted_iota(jnp.int32, (128, ROWS), 0) + blk * 128
        perm[pl.ds(blk * 128, 128), :] = jnp.where(rows == dest_i, 1.0, 0.0).astype(BF16)

    def send_k(half):
        for h in range(2):
            for t, tchip in enumerate((xchip, ychip)):
                rcopy(kst.at[h, half], kbuf.at[1 + t, core, half], s_k, r_k.at[t, half], 2 * tchip + h).start()

    def split_v(src, slot):
        f_scr[pl.ds(0, 2 * ROWS), :] = src[...].astype(F32)
        for mine in range(2):
            h = core if mine else other
            vt = f_scr[pl.ds(h, ROWS, stride=2), :].T.astype(BF16)
            vc = nt(vt, perm[...]).astype(BF16)
            for half in range(2):
                part = vc[:, half * HALF:(half + 1) * HALF]
                if mine:
                    vbuf[slot, core, half] = part
                else:
                    vst[slot, half] = part
        rcopy(vst.at[slot], vbuf.at[slot, core], s_share if slot else s_own, r_share.at[0] if slot else r_own.at[0], partner).start()

    in_copies[2].wait()
    in_copies[5].wait()
    angle = freq_v[...] * pos_v[...].astype(F32)
    cs_scr[0] = jnp.cos(angle)
    cs_scr[1] = jnp.sin(angle)

    def norm_rope(rows_f32, gain_v):
        xt = rows_f32.T
        inv = lax.rsqrt(jnp.mean(xt * xt, axis=0, keepdims=True) + EPS)
        gain = jnp.broadcast_to(gain_v[...].astype(F32), (128, D)).T
        gain = jnp.concatenate([gain] * 4, axis=1)
        n = (xt * inv * gain).astype(BF16).astype(F32)
        a, b = n[:64], n[64:]
        cos, sin = cs_scr[0], cs_scr[1]
        return jnp.concatenate([a * cos - b * sin, b * cos + a * sin], axis=0).astype(BF16)

    in_copies[3].wait()
    in_copies[4].wait()
    f_scr[pl.ds(0, 1024), :] = k_in[...].astype(F32)
    for h in range(2):
        kr = norm_rope(f_scr[pl.ds(h, ROWS, stride=2), :], kg_v)
        kc = nt(perm[...], kr).astype(BF16)
        for half in range(2):
            kst[h, half] = kc[half * HALF:(half + 1) * HALF, :]
    for half in range(2):
        kbuf[0, core, half] = kst[core, half]

    send_k(0)
    send_k(1)
    rcopy(kst.at[other], kbuf.at[0, core], s_own, r_own.at[0], partner).start()

    in_copies[0].wait()
    split_v(v_in, 0)

    in_copies[6].wait()
    in_copies[7].wait()
    f_scr[...] = q_in[...].astype(F32)

    def q_head(h, store):
        qr = norm_rope(f_scr[pl.ds(h, ROWS, stride=4), :], qg_v)
        qc = nt(qr, perm[...]).astype(BF16)
        for half in range(2):
            store(half, qc[:, half * HALF:(half + 1) * HALF])

    for g in range(2):
        def store_other(half, val, g=g):
            qst[half, :, g * HALF:(g + 1) * HALF] = val
        q_head(2 * other + g, store_other)
    rcopy(qst, qbuf.at[:, 0, pl.ds(0, D), :], s_own, r_own.at[0], partner).start()
    for g in range(2):
        def store_own(half, val, g=g):
            qbuf[half, 1, pl.ds(0, D), g * HALF:(g + 1) * HALF] = val
        q_head(2 * core + g, store_own)

    lane_d = lax.broadcasted_iota(jnp.int32, (8, HALF), 1).astype(F32)
    in_run = (lane_d >= start * 0.5) & (lane_d < (start + cnt) * 0.5)
    one_hot = jnp.where(in_run, 1.0, 0.0)
    blocked = jnp.where(in_run, 0.0, NEG_BIG)
    blocked = jnp.where(lax.broadcasted_iota(jnp.int32, (8, HALF), 0) < 4, blocked, 0.0)
    pad = jnp.zeros((D - 8, HALF), F32)
    q_extra = jnp.concatenate([blocked, pad], axis=0).astype(BF16)
    for half in range(2):
        for dev in range(2):
            for g in range(2):
                qbuf[half, dev, pl.ds(D, D), g * HALF:(g + 1) * HALF] = q_extra
    kaug[...] = jnp.concatenate([one_hot, pad], axis=0).T.astype(BF16)

    dest_cols = jnp.broadcast_to(dest, (128, ROWS)).T.astype(jnp.int32)
    for blk in range(4):
        lanes = lax.broadcasted_iota(jnp.int32, (ROWS, 128), 1) + blk * 128
        perm_t[blk // 2, :, (blk % 2) * 128:(blk % 2 + 1) * 128] = jnp.where(lanes == dest_cols, 1.0, 0.0).astype(BF16)

    m_scr[...] = jnp.full(m_scr.shape, NEG_BIG, F32)
    l_scr[...] = jnp.zeros(l_scr.shape, F32)
    acc[...] = jnp.zeros(acc.shape, F32)

    def tile_parts(slot, khalf, qhalf, causal):
        ka = kaug[...]
        keys = [jnp.concatenate([kbuf[slot, dev, khalf], ka], axis=1) for dev in range(2)]
        keys = jnp.concatenate(keys, axis=0)
        v0 = vbuf[slot, 0, khalf]
        v1 = vbuf[slot, 1, khalf]
        chunks = [(dev, g) for dev in range(2) for g in range(2)]

        def scores(n):
            dev, g = chunks[n]
            s = nn(keys, qbuf[qhalf, dev, :, pl.ds(g * HALF, HALF)])
            if causal:
                abs_dev = core if dev == 1 else other
                krow = lax.broadcasted_iota(jnp.int32, (2 * HALF, HALF), 0)
                qcol = lax.broadcasted_iota(jnp.int32, (2 * HALF, HALF), 1)
                kord = krow + qhalf * jnp.where(krow < HALF, HALF, -HALF)
                qord = qcol + (abs_dev + qhalf * (1 - 2 * abs_dev)) * HALF
                s = jnp.where(kord <= qord, s, NEG_BIG)
            return s

        def soft(n, s):
            dev, g = chunks[n]
            cols = pl.ds(g * HALF, HALF)
            m_old = m_scr[qhalf, dev, :, cols]
            m_new = jnp.maximum(m_old, jnp.max(s, axis=0, keepdims=True))
            p = jnp.exp2((s - m_new) * C_EXP)
            alpha = jnp.exp2((m_old - m_new) * C_EXP)
            m_scr[qhalf, dev, :, cols] = m_new
            l_scr[qhalf, dev, :, cols] = l_scr[qhalf, dev, :, cols] * alpha + jnp.sum(p, axis=0, keepdims=True)
            return p.astype(BF16), alpha

        def out(n, pb, alpha):
            dev, g = chunks[n]
            cols = pl.ds(g * HALF, HALF)
            o = nn(v0, pb[:HALF]) + nn(v1, pb[HALF:])
            acc[qhalf, dev, :, cols] = acc[qhalf, dev, :, cols] * alpha + o

        return scores, soft, out

    def tile(slot, khalf, qhalf, causal):
        scores, soft, out = tile_parts(slot, khalf, qhalf, causal)
        s = scores(0)
        prev = None
        for n in range(4):
            nxt = scores(n + 1) if n < 3 else None
            pb, alpha = soft(n, s)
            if prev is not None:
                out(n - 1, *prev)
            prev = (pb, alpha)
            s = nxt
        out(3, *prev)

    arrived(r_own.at[0], 512)

    def own_body(half, carry):
        tile(0, half, half, True)
        return carry

    lax.fori_loop(0, 2, own_body, 0)

    def fwd_v(dev, half):
        slot, to = (2, xchip) if dev == 0 else (1, ychip)
        return rcopy(vbuf.at[slot, dev, half], vbuf.at[3, dev, half], s_fwd, r_far.at[2 * half], 2 * to + core)

    def fwd_k(dev, half):
        slot, to = (2, xchip) if dev == 0 else (1, ychip)
        return rcopy(kbuf.at[slot, dev, half], kbuf.at[3, dev, half], s_fwd, r_far.at[half], 2 * to + core)

    def body(idx, carry):
        @pl.when(idx == 1)
        def _():
            for t in range(2):
                raw_v(t).wait_recv()
                split_v(vraw.at[t], 1 + t)
            arrived(r_share.at[0], 256)
            for dev in range(2):
                fwd_v(dev, 0).start()
            for t in range(2):
                arrived(r_k.at[t, 0], 128)
                fwd_k(1 - t, 0).start()

        @pl.when(idx == 3)
        def _():
            for t in range(2):
                arrived(r_k.at[t, 1], 128)
                fwd_k(1 - t, 1).start()
            for dev in range(2):
                fwd_v(dev, 1).start()

        @pl.when(idx == 5)
        def _():
            arrived(r_far.at[0], 256)

        second = (idx // 3) * (1 - idx // 5)
        slot = idx - 2 * second - 2 * (idx // 5)
        late_needed = (1 - y) + (idx % 2) * (y - x)
        sel = second * late_needed
        tile(slot, sel, 1 - second + sel, False)
        return carry

    lax.fori_loop(0, 6, body, 0)

    done = y
    last = 1 - y

    def place(grp, half, first):
        for g in range(2):
            rows = pl.ds(2 * grp + g, ROWS, stride=4)
            val = nt(perm_t[half], obuf[grp, half, g])
            f_scr[rows, :] = val if first else f_scr[rows, :] + val

    def give(half, n):
        return rcopy(ost.at[half], obuf.at[core, half], s_o, r_o.at[n], partner)

    def take(half, n):
        rcopy(ost.at[half], obuf.at[other, half], s_o, r_o.at[n], partner).wait_recv()

    for g in range(2):
        cols = pl.ds(g * HALF, HALF)
        ost[done, g] = (acc[done, 0, :, cols] * (1.0 / l_scr[done, 0, :, cols])).astype(BF16)
    give(done, 0).start()
    for g in range(2):
        cols = pl.ds(g * HALF, HALF)
        obuf[core, done, g] = (acc[done, 1, :, cols] * (1.0 / l_scr[done, 1, :, cols])).astype(BF16)
    place(core, done, True)

    arrived(r_far.at[1], 128)
    scores, soft, _ = tile_parts(3, last, last, False)
    s = scores(0)
    for n in range(4):
        nxt = scores(n + 1) if n < 3 else None
        pb, alpha = soft(n, s)
        pbuf[n] = pb
        cols = pl.ds((n % 2) * HALF, HALF)
        acc[last, n // 2, :, cols] = acc[last, n // 2, :, cols] * alpha
        s = nxt
    for dev in range(2):
        for half in range(2):
            for g in range(2):
                cols = pl.ds(g * HALF, HALF)
                val = m_scr[half, dev, :, cols] * SCALE + jnp.log(l_scr[half, dev, :, cols])
                if dev == 0:
                    lst[pl.ds(g, 1), half * HALF:(half + 1) * HALF] = val
                else:
                    lbuf[core, pl.ds(g, 1), half * HALF:(half + 1) * HALF] = val
        if dev == 0:
            l_send = rcopy(lst, lbuf.at[core], s_l, r_l.at[0], partner)
            l_send.start()
    take(done, 0)
    place(other, done, True)

    arrived(r_far.at[2], 128)
    for n in range(4):
        cols = pl.ds((n % 2) * HALF, HALF)
        dev, g = n // 2, n % 2
        o = nn(vbuf[3, 0, last], pbuf[n, :HALF, :]) + nn(vbuf[3, 1, last], pbuf[n, HALF:, :])
        o = ((acc[last, dev, :, cols] + o) * (1.0 / l_scr[last, dev, :, cols])).astype(BF16)
        if dev == 0:
            ost[last, g] = o
        else:
            obuf[core, last, g] = o
        if n == 1:
            give(last, 1).start()
    place(core, last, False)
    rcopy(lst, lbuf.at[other], s_l, r_l.at[0], partner).wait_recv()
    lse = jnp.concatenate([lbuf[0, :2], lbuf[1, :2]], axis=0)
    hi = lse.astype(BF16).astype(F32)
    rest = lse - hi
    mid = rest.astype(BF16).astype(F32)
    pieces = jnp.concatenate([hi, mid, rest - mid, jnp.zeros((4, ROWS), F32)], axis=0).astype(BF16)
    pieces = nn(pieces, perm[...])
    lse_out[...] = pieces[0:4] + pieces[4:8] + pieces[8:12]
    for sem, kib in ((s_raw.at[0], 512), (s_k, 512), (s_own, 512), (s_share, 256), (s_fwd, 512)):
        sent(sem, kib)
    l_send.wait_send()
    take(last, 1)
    place(other, last, False)
    out_ref[...] = f_scr[...].astype(BF16)

    sent(s_o, 256)


def write_out(o_ref, l_ref, o_hbm, l_hbm, sem):
    copies = [pltpu.make_async_copy(o_ref, o_hbm, sem.at[0]), pltpu.make_async_copy(l_ref, l_hbm, sem.at[1])]
    for cp in copies:
        cp.start()
    for cp in copies:
        cp.wait()


def solution(mesh):
    freq = (THETA ** (-(np.arange(64, dtype=np.float64) * 2.0) / D)).astype(np.float32)
    freq = np.broadcast_to(freq[:, None], (64, ROWS)).copy()
    any_spec = pl.BlockSpec(memory_space=pl.ANY)
    dma = pltpu.SemaphoreType.DMA
    vm = pltpu.VMEM

    def per_device(q_raw, k_raw, v_raw, positions, seq_ids, q_gain, k_gain):
        call = pl.pallas_call(
            kernel,
            out_shape=(jax.ShapeDtypeStruct((4 * ROWS, D), BF16), jax.ShapeDtypeStruct((4, ROWS), F32)),
            in_specs=[any_spec] * 8,
            out_specs=(pl.BlockSpec(memory_space=pltpu.VMEM), pl.BlockSpec(memory_space=pltpu.VMEM)),
            scratch_shapes=[
                vm((4 * ROWS, D), BF16), vm((2 * ROWS, D), BF16), vm((2 * ROWS, D), BF16),
                vm((1, ROWS), jnp.int32), vm((1, ROWS), jnp.int32), vm((1, D), BF16), vm((1, D), BF16),
                vm((64, ROWS), F32),
                vm((4 * ROWS, D), F32), vm((2, 64, ROWS), F32), vm((ROWS, ROWS), BF16), vm((2, ROWS, HALF), BF16),
                vm((4, 2, 2, HALF, D), BF16), vm((4, 2, 2, D, HALF), BF16),
                vm((2, 2 * ROWS, D), BF16), vm((2, 2, HALF, D), BF16), vm((3, 2, D, HALF), BF16),
                vm((2, 2, 2 * D, 2 * HALF), BF16), vm((2, D, 2 * HALF), BF16), vm((HALF, D), BF16),
                vm((2, 2, 1, 2 * HALF), F32), vm((2, 2, 1, 2 * HALF), F32), vm((2, 2, D, 2 * HALF), F32),
                vm((2, 2, D, HALF), BF16), vm((2, 2, 2, D, HALF), BF16), vm((8, ROWS), F32), vm((2, 8, ROWS), F32),
                vm((4, 2 * HALF, HALF), BF16),
                dma((8,)), pltpu.SemaphoreType.REGULAR, dma((1,)), dma((2,)), dma((1,)), dma((1,)), dma((2, 2)), dma((3,)), dma((2,)), dma((1,)),
            ],
            compiler_params=pltpu.CompilerParams(collective_id=0, has_side_effects=True, vmem_limit_bytes=40000 * 1024),
        )
        args = (q_raw.reshape(4 * ROWS, D), k_raw.reshape(2 * ROWS, D), v_raw.reshape(2 * ROWS, D),
                positions.reshape(1, ROWS), seq_ids.reshape(1, ROWS), q_gain.reshape(1, D), k_gain.reshape(1, D),
                jnp.asarray(freq))
        args = [pltpu.with_memory_space_constraint(a, pltpu.HBM) for a in args]
        out, lse = call(*args)
        out, lse = pl.pallas_call(
            write_out,
            out_shape=(jax.ShapeDtypeStruct((4 * ROWS, D), BF16), jax.ShapeDtypeStruct((4, ROWS), F32)),
            in_specs=[pl.BlockSpec(memory_space=pltpu.VMEM)] * 2,
            out_specs=(pl.BlockSpec(memory_space=pltpu.HBM), pl.BlockSpec(memory_space=pltpu.HBM)),
            scratch_shapes=[dma((2,))],
            compiler_params=pltpu.CompilerParams(vmem_limit_bytes=1024*1024),
        )(out, lse)
        return out.reshape(ROWS, 4, D), lse.T

    return jax.shard_map(per_device, mesh=mesh, in_specs=(P("cp", "tp", None), P("cp", "tp", None), P("cp", "tp", None), P("cp"), P("cp"), P(), P()), out_specs=(P("cp", "tp", None), P("cp", "tp")), check_vma=False)
```

```python
import functools
import math

import jax
import jax.numpy as jnp
import numpy as np
from jax import lax
from jax.experimental import pallas as pl
from jax.experimental.pallas import tpu as pltpu
from jax.sharding import PartitionSpec as P

THETA = 1000000.0
EPS = 1e-6
NEG_BIG = -1e30
D = 128
HALF = 256
ROWS = 512
C_EXP = (D ** -0.5) * math.log2(math.e)
SCALE = D ** -0.5
F32 = jnp.float32
BF16 = jnp.bfloat16


def nt(a, b):
    return lax.dot_general(a, b, (((1,), (1,)), ((), ())), preferred_element_type=F32)


def nn(a, b):
    return lax.dot_general(a, b, (((1,), (0,)), ((), ())), preferred_element_type=F32)


def kernel(q_hbm, k_hbm, v_hbm, pos_hbm, seq_hbm, qg_hbm, kg_hbm, freq_hbm, out_ref, lse_out, lay_ref,
           q_in, k_in, v_in, pos_v, seq_v, qg_v, kg_v, freq_v, f_scr, cs_scr, perm,
           kbuf, vbuf, vraw, kst, vst, qbuf, qst, kaug, m_scr, l_scr, acc, ost, obuf, lst, lbuf, pbuf, abuf,
           in_sem, ready, s_raw, r_raw, r_own, r_share, r_k, r_far, r_o, r_l):
    me = lax.axis_index("cp")
    core = lax.rem(me, 2)
    chip = lax.div(me, 2)
    x = lax.rem(chip, 2)
    y = lax.div(chip, 2)
    xchip = chip + 1 - 2 * x
    ychip = chip + 2 - 4 * y
    other = 1 - core
    partner = 2 * chip + other

    def rcopy(src, dst, ssem, rsem, dev):
        return pltpu.make_async_remote_copy(src_ref=src, dst_ref=dst, send_sem=ssem, recv_sem=rsem,
                                            device_id={"cp": dev}, device_id_type=pl.DeviceIdType.MESH)

    s_k, s_own, s_share, s_fwd, s_o, s_l = (in_sem.at[n] for n in (1, 2, 3, 4, 5, 0))

    def sized(kib):
        return kbuf.at[pl.ds(0, kib // 256)] if kib >= 256 else kbuf.at[0, pl.ds(0, kib // 128)]

    def sent(sem, kib):
        rcopy(sized(kib), sized(kib), sem, r_l.at[0], partner).wait_send()

    def arrived(sem, kib):
        rcopy(sized(kib), sized(kib), s_l, sem, partner).wait_recv()

    barrier = pltpu.get_barrier_semaphore()
    for peer in (2 * xchip, 2 * ychip + 1, partner):
        pl.semaphore_signal(barrier, inc=1, device_id={"cp": peer}, device_id_type=pl.DeviceIdType.MESH)

    ins = [(v_hbm, v_in), (seq_hbm, seq_v), (pos_hbm, pos_v), (k_hbm, k_in), (kg_hbm, kg_v), (freq_hbm, freq_v),
           (q_hbm, q_in), (qg_hbm, qg_v)]
    in_copies = [pltpu.make_async_copy(src, dst, in_sem.at[n]) for n, (src, dst) in enumerate(ins)]
    for n in (1, 2, 5, 3, 4, 0, 6, 7):
        in_copies[n].start()

    pl.semaphore_wait(barrier, 3)
    pl.semaphore_signal(ready, inc=1, device_id={"cp": partner}, device_id_type=pl.DeviceIdType.MESH)

    def raw_v(t):
        tchip = xchip + t * (ychip - xchip)
        return rcopy(v_hbm, vraw.at[t], s_raw.at[0], r_raw.at[t], 2 * tchip + core)

    raw_v(core).start()
    pl.semaphore_wait(ready, 1)
    raw_v(other).start()

    in_copies[1].wait()
    seq = seq_v[...]
    row_id = lax.broadcasted_iota(jnp.int32, (8, ROWS), 1).astype(F32)
    sub_id = lax.broadcasted_iota(jnp.int32, (8, ROWS), 0)
    is_seq = jnp.broadcast_to(seq, (8, ROWS)) == sub_id
    seq_f = jnp.where(is_seq, 1.0, 0.0)
    cnt = jnp.sum(seq_f, axis=1, keepdims=True)
    start = jnp.min(jnp.where(is_seq, row_id, float(ROWS)), axis=1, keepdims=True)
    start_row = jnp.sum(seq_f * start, axis=0, keepdims=True)
    cnt_row = jnp.sum(seq_f * cnt, axis=0, keepdims=True)
    off = row_id[:1] - start_row
    late = off * 2.0 >= cnt_row
    dest = start_row * 0.5 + off + jnp.where(late, HALF - 0.5 * cnt_row, 0.0)
    dest_i = dest.astype(jnp.int32)
    for blk in range(4):
        rows = lax.broadcasted_iota(jnp.int32, (128, ROWS), 0) + blk * 128
        perm[pl.ds(blk * 128, 128), :] = jnp.where(rows == dest_i, 1.0, 0.0).astype(BF16)

    def send_k(half):
        for h in range(2):
            for t, tchip in enumerate((xchip, ychip)):
                rcopy(kst.at[h, half], kbuf.at[1 + t, core, half], s_k, r_k.at[t, half], 2 * tchip + h).start()

    def split_v(src, slot):
        f_scr[pl.ds(0, 2 * ROWS), :] = src[...].astype(F32)
        for mine in range(2):
            h = core if mine else other
            vt = f_scr[pl.ds(h, ROWS, stride=2), :].T.astype(BF16)
            vc = nt(vt, perm[...]).astype(BF16)
            for half in range(2):
                part = vc[:, half * HALF:(half + 1) * HALF]
                if mine:
                    vbuf[slot, core, half] = part
                else:
                    vst[slot, half] = part
        rcopy(vst.at[slot], vbuf.at[slot, core], s_share if slot else s_own, r_share.at[0] if slot else r_own.at[0], partner).start()

    in_copies[2].wait()
    in_copies[5].wait()
    angle = freq_v[...] * pos_v[...].astype(F32)
    cs_scr[0] = jnp.cos(angle)
    cs_scr[1] = jnp.sin(angle)

    def norm_rope(rows_f32, gain_v):
        xt = rows_f32.T
        inv = lax.rsqrt(jnp.mean(xt * xt, axis=0, keepdims=True) + EPS)
        gain = jnp.broadcast_to(gain_v[...].astype(F32), (128, D)).T
        gain = jnp.concatenate([gain] * 4, axis=1)
        n = (xt * inv * gain).astype(BF16).astype(F32)
        a, b = n[:64], n[64:]
        cos, sin = cs_scr[0], cs_scr[1]
        return jnp.concatenate([a * cos - b * sin, b * cos + a * sin], axis=0).astype(BF16)

    in_copies[3].wait()
    in_copies[4].wait()
    f_scr[pl.ds(0, 1024), :] = k_in[...].astype(F32)
    for h in range(2):
        kr = norm_rope(f_scr[pl.ds(h, ROWS, stride=2), :], kg_v)
        kc = nt(perm[...], kr).astype(BF16)
        for half in range(2):
            kst[h, half] = kc[half * HALF:(half + 1) * HALF, :]
    for half in range(2):
        kbuf[0, core, half] = kst[core, half]

    send_k(0)
    send_k(1)
    rcopy(kst.at[other], kbuf.at[0, core], s_own, r_own.at[0], partner).start()

    in_copies[0].wait()
    split_v(v_in, 0)

    in_copies[6].wait()
    in_copies[7].wait()
    f_scr[...] = q_in[...].astype(F32)

    def q_head(h, store):
        qr = norm_rope(f_scr[pl.ds(h, ROWS, stride=4), :], qg_v)
        qc = nt(qr, perm[...]).astype(BF16)
        for half in range(2):
            store(half, qc[:, half * HALF:(half + 1) * HALF])

    for g in range(2):
        def store_other(half, val, g=g):
            qst[half, :, g * HALF:(g + 1) * HALF] = val
        q_head(2 * other + g, store_other)
    rcopy(qst, qbuf.at[:, 0, pl.ds(0, D), :], s_own, r_own.at[0], partner).start()
    for g in range(2):
        def store_own(half, val, g=g):
            qbuf[half, 1, pl.ds(0, D), g * HALF:(g + 1) * HALF] = val
        q_head(2 * core + g, store_own)

    lane_d = lax.broadcasted_iota(jnp.int32, (8, HALF), 1).astype(F32)
    in_run = (lane_d >= start * 0.5) & (lane_d < (start + cnt) * 0.5)
    one_hot = jnp.where(in_run, 1.0, 0.0)
    blocked = jnp.where(in_run, 0.0, NEG_BIG)
    blocked = jnp.where(lax.broadcasted_iota(jnp.int32, (8, HALF), 0) < 4, blocked, 0.0)
    pad = jnp.zeros((D - 8, HALF), F32)
    q_extra = jnp.concatenate([blocked, pad], axis=0).astype(BF16)
    for half in range(2):
        for dev in range(2):
            for g in range(2):
                qbuf[half, dev, pl.ds(D, D), g * HALF:(g + 1) * HALF] = q_extra
    kaug[...] = jnp.concatenate([one_hot, pad], axis=0).T.astype(BF16)

    lane_l = lax.broadcasted_iota(jnp.int32, (8, D), 1)
    lay_ref[...] = jnp.where(lane_l == 0, start, cnt * 0.5).astype(jnp.int32)

    m_scr[...] = jnp.full(m_scr.shape, NEG_BIG, F32)
    l_scr[...] = jnp.zeros(l_scr.shape, F32)
    acc[...] = jnp.zeros(acc.shape, F32)

    def tile_parts(slot, khalf, qhalf, causal):
        ka = kaug[...]
        keys = [jnp.concatenate([kbuf[slot, dev, khalf], ka], axis=1) for dev in range(2)]
        keys = jnp.concatenate(keys, axis=0)
        v0 = vbuf[slot, 0, khalf]
        v1 = vbuf[slot, 1, khalf]
        chunks = [(dev, g) for dev in range(2) for g in range(2)]

        def scores(n):
            dev, g = chunks[n]
            s = nn(keys, qbuf[qhalf, dev, :, pl.ds(g * HALF, HALF)])
            if causal:
                abs_dev = core if dev == 1 else other
                krow = lax.broadcasted_iota(jnp.int32, (2 * HALF, HALF), 0)
                qcol = lax.broadcasted_iota(jnp.int32, (2 * HALF, HALF), 1)
                kord = krow + qhalf * jnp.where(krow < HALF, HALF, -HALF)
                qord = qcol + (abs_dev + qhalf * (1 - 2 * abs_dev)) * HALF
                s = jnp.where(kord <= qord, s, NEG_BIG)
            return s

        def soft(n, s):
            dev, g = chunks[n]
            cols = pl.ds(g * HALF, HALF)
            m_old = m_scr[qhalf, dev, :, cols]
            m_new = jnp.maximum(m_old, jnp.max(s, axis=0, keepdims=True))
            p = jnp.exp2((s - m_new) * C_EXP)
            alpha = jnp.exp2((m_old - m_new) * C_EXP)
            m_scr[qhalf, dev, :, cols] = m_new
            l_scr[qhalf, dev, :, cols] = l_scr[qhalf, dev, :, cols] * alpha + jnp.sum(p, axis=0, keepdims=True)
            return p.astype(BF16), alpha

        def out(n, pb, alpha):
            dev, g = chunks[n]
            cols = pl.ds(g * HALF, HALF)
            o = nn(v0, pb[:HALF]) + nn(v1, pb[HALF:])
            acc[qhalf, dev, :, cols] = acc[qhalf, dev, :, cols] * alpha + o

        return scores, soft, out

    def tile(slot, khalf, qhalf, causal):
        scores, soft, out = tile_parts(slot, khalf, qhalf, causal)
        s = scores(0)
        prev = None
        for n in range(4):
            nxt = scores(n + 1) if n < 3 else None
            pb, alpha = soft(n, s)
            if prev is not None:
                out(n - 1, *prev)
            prev = (pb, alpha)
            s = nxt
        out(3, *prev)

    arrived(r_own.at[0], 512)

    def own_body(half, carry):
        tile(0, half, half, True)
        return carry

    lax.fori_loop(0, 2, own_body, 0)

    def fwd_v(dev, half):
        slot, to = (2, xchip) if dev == 0 else (1, ychip)
        return rcopy(vbuf.at[slot, dev, half], vbuf.at[3, dev, half], s_fwd, r_far.at[half, 1], 2 * to + core)

    def fwd_k(dev, half):
        slot, to = (2, xchip) if dev == 0 else (1, ychip)
        return rcopy(kbuf.at[slot, dev, half], kbuf.at[3, dev, half], s_fwd, r_far.at[half, 0], 2 * to + core)

    done = y
    last = 1 - y

    def place(grp, half):
        for g in range(2):
            f_scr[pl.ds(half * 4 * HALF + 2 * grp + g, HALF, stride=4), :] = obuf[grp, half, g].astype(F32)

    def pack(half):
        rows = pl.ds(pl.multiple_of(half * 4 * HALF, 4 * HALF), 4 * HALF)
        out_ref[rows, :] = f_scr[rows, :].astype(BF16)

    def give(half, n):
        return rcopy(ost.at[half], obuf.at[core, half], s_o, r_o.at[n], partner)

    def take(half, n):
        rcopy(ost.at[half], obuf.at[other, half], s_o, r_o.at[n], partner).wait_recv()

    def early(half):
        for g in range(2):
            cols = pl.ds(g * HALF, HALF)
            ost[half, g] = (acc[half, 0, :, cols] * (1.0 / l_scr[half, 0, :, cols])).T.astype(BF16)
        give(half, 0).start()
        for g in range(2):
            cols = pl.ds(g * HALF, HALF)
            obuf[core, half, g] = (acc[half, 1, :, cols] * (1.0 / l_scr[half, 1, :, cols])).T.astype(BF16)
        place(core, half)

    def take_early(half):
        take(half, 0)
        place(other, half)
        pack(half)

    def body(idx, carry):
        @pl.when(idx == 1)
        def _():
            for t in range(2):
                raw_v(t).wait_recv()
                split_v(vraw.at[t], 1 + t)
            arrived(r_share.at[0], 256)
            for t in range(2):
                arrived(r_k.at[t, 0], 128)
                fwd_k(1 - t, 0).start()
            for dev in range(2):
                fwd_v(dev, 0).start()

        @pl.when(idx == 3)
        def _():
            for t in range(2):
                arrived(r_k.at[t, 1], 128)
                fwd_k(1 - t, 1).start()
            for dev in range(2):
                fwd_v(dev, 1).start()

        @pl.when((idx == 4) & (y == 0))
        def _():
            early(0)

        second = idx // 3
        slot = idx - 2 * second
        late_needed = (1 - y) + (idx % 2) * (y - x)
        sel = second * late_needed
        tile(slot, sel, 1 - second + sel, False)
        return carry

    lax.fori_loop(0, 5, body, 0)

    def weigh(khalf, qhalf):
        scores, soft, _ = tile_parts(3, khalf, qhalf, False)
        s = scores(0)
        for n in range(4):
            nxt = scores(n + 1) if n < 3 else None
            pb, alpha = soft(n, s)
            pbuf[n] = pb
            abuf[n] = alpha
            s = nxt

    def weighted(n, khalf):
        return nn(vbuf[3, 0, khalf], pbuf[n, :HALF, :]) + nn(vbuf[3, 1, khalf], pbuf[n, HALF:, :])

    @pl.when(y == 0)
    def _():
        take_early(0)

    arrived(r_far.at[0, 0], 128)
    weigh(0, 1)
    arrived(r_far.at[0, 1], 128)
    for n in range(4):
        cols = pl.ds((n % 2) * HALF, HALF)
        acc[1, n // 2, :, cols] = acc[1, n // 2, :, cols] * abuf[n] + weighted(n, 0)

    @pl.when(y == 1)
    def _():
        early(1)

    arrived(r_far.at[1, 0], 128)
    weigh(last, last)
    for dev in range(2):
        for half in range(2):
            for g in range(2):
                cols = pl.ds(g * HALF, HALF)
                val = m_scr[half, dev, :, cols] * SCALE + jnp.log(l_scr[half, dev, :, cols])
                if dev == 0:
                    lst[pl.ds(g, 1), half * HALF:(half + 1) * HALF] = val
                else:
                    lbuf[core, pl.ds(g, 1), half * HALF:(half + 1) * HALF] = val
        if dev == 0:
            l_send = rcopy(lst, lbuf.at[core], s_l, r_l.at[0], partner)
            l_send.start()
    @pl.when(y == 1)
    def _():
        take_early(1)

    arrived(r_far.at[1, 1], 128)
    for n in range(4):
        cols = pl.ds((n % 2) * HALF, HALF)
        dev, g = n // 2, n % 2
        o = ((acc[last, dev, :, cols] * abuf[n] + weighted(n, last)) * (1.0 / l_scr[last, dev, :, cols])).T.astype(BF16)
        if dev == 0:
            ost[last, g] = o
        else:
            obuf[core, last, g] = o
        if n == 1:
            give(last, 1).start()
    place(core, last)
    rcopy(lst, lbuf.at[other], s_l, r_l.at[0], partner).wait_recv()
    lse = jnp.concatenate([lbuf[0, :2], lbuf[1, :2]], axis=0)
    hi = lse.astype(BF16).astype(F32)
    rest = lse - hi
    mid = rest.astype(BF16).astype(F32)
    pieces = jnp.concatenate([hi, mid, rest - mid, jnp.zeros((4, ROWS), F32)], axis=0).astype(BF16)
    pieces = nn(pieces, perm[...])
    lse_out[...] = pieces[0:4] + pieces[4:8] + pieces[8:12]
    for sem, kib in ((s_raw.at[0], 512), (s_k, 512), (s_own, 512), (s_share, 256), (s_fwd, 512)):
        sent(sem, kib)
    l_send.wait_send()
    take(last, 1)
    place(other, last)
    pack(last)

    sent(s_o, 256)


def write_out(o_ref, l_ref, lay_ref, o_hbm, l_hbm, sem):
    lse_copy = pltpu.make_async_copy(l_ref, l_hbm, sem.at[1])
    lse_copy.start()
    lay = lay_ref[...]
    for seq in range(4):
        first, piece = lay[seq, 0], lay[seq, 1]
        for half in range(2):
            src = o_ref.at[pl.ds(half * HALF + first // 2, piece)]
            pltpu.make_async_copy(src, o_hbm.at[pl.ds(first + half * piece, piece)], sem.at[0]).start()
    pltpu.make_async_copy(o_ref, o_hbm, sem.at[0]).wait()
    lse_copy.wait()


def solution(mesh):
    freq = (THETA ** (-(np.arange(64, dtype=np.float64) * 2.0) / D)).astype(np.float32)
    freq = np.broadcast_to(freq[:, None], (64, ROWS)).copy()
    any_spec = pl.BlockSpec(memory_space=pl.ANY)
    dma = pltpu.SemaphoreType.DMA
    vm = pltpu.VMEM

    def per_device(q_raw, k_raw, v_raw, positions, seq_ids, q_gain, k_gain):
        call = pl.pallas_call(
            kernel,
            out_shape=(jax.ShapeDtypeStruct((4 * ROWS, D), BF16), jax.ShapeDtypeStruct((4, ROWS), F32), jax.ShapeDtypeStruct((8, D), jnp.int32)),
            in_specs=[any_spec] * 8,
            out_specs=(pl.BlockSpec(memory_space=pltpu.VMEM),) * 3,
            scratch_shapes=[
                vm((4 * ROWS, D), BF16), vm((2 * ROWS, D), BF16), vm((2 * ROWS, D), BF16),
                vm((1, ROWS), jnp.int32), vm((1, ROWS), jnp.int32), vm((1, D), BF16), vm((1, D), BF16),
                vm((64, ROWS), F32),
                vm((4 * ROWS, D), F32), vm((2, 64, ROWS), F32), vm((ROWS, ROWS), BF16),
                vm((4, 2, 2, HALF, D), BF16), vm((4, 2, 2, D, HALF), BF16),
                vm((2, 2 * ROWS, D), BF16), vm((2, 2, HALF, D), BF16), vm((3, 2, D, HALF), BF16),
                vm((2, 2, 2 * D, 2 * HALF), BF16), vm((2, D, 2 * HALF), BF16), vm((HALF, D), BF16),
                vm((2, 2, 1, 2 * HALF), F32), vm((2, 2, 1, 2 * HALF), F32), vm((2, 2, D, 2 * HALF), F32),
                vm((2, 2, HALF, D), BF16), vm((2, 2, 2, HALF, D), BF16), vm((8, ROWS), F32), vm((2, 8, ROWS), F32),
                vm((4, 2 * HALF, HALF), BF16), vm((4, 1, HALF), F32),
                dma((8,)), pltpu.SemaphoreType.REGULAR, dma((1,)), dma((2,)), dma((1,)), dma((1,)), dma((2, 2)), dma((2, 2)), dma((2,)), dma((1,)),
            ],
            compiler_params=pltpu.CompilerParams(collective_id=0, has_side_effects=True, vmem_limit_bytes=40000 * 1024),
        )
        args = (q_raw.reshape(4 * ROWS, D), k_raw.reshape(2 * ROWS, D), v_raw.reshape(2 * ROWS, D),
                positions.reshape(1, ROWS), seq_ids.reshape(1, ROWS), q_gain.reshape(1, D), k_gain.reshape(1, D),
                jnp.asarray(freq))
        args = [pltpu.with_memory_space_constraint(a, pltpu.HBM) for a in args]
        out, lse, lay = call(*args)
        out, lse = pl.pallas_call(
            write_out,
            out_shape=(jax.ShapeDtypeStruct((ROWS, 4, D), BF16), jax.ShapeDtypeStruct((4, ROWS), F32)),
            in_specs=[pl.BlockSpec(memory_space=pltpu.VMEM)] * 3,
            out_specs=(pl.BlockSpec(memory_space=pltpu.HBM), pl.BlockSpec(memory_space=pltpu.HBM)),
            scratch_shapes=[dma((2,))],
            compiler_params=pltpu.CompilerParams(vmem_limit_bytes=1024 * 1024),
        )(out.reshape(ROWS, 4, D), lse, lay)
        return out, lse.T

    return jax.shard_map(per_device, mesh=mesh, in_specs=(P("cp", "tp", None), P("cp", "tp", None), P("cp", "tp", None), P("cp"), P("cp"), P(), P()), out_specs=(P("cp", "tp", None), P("cp", "tp")), check_vma=False)
```

```python
import math

import jax
import jax.numpy as jnp
import numpy as np
from jax import lax
from jax.experimental import pallas as pl
from jax.experimental.pallas import tpu as pltpu
from jax.sharding import PartitionSpec as P

THETA = 1000000.0
EPS = 1e-6
NEG_BIG = -1e30
D = 128
HALF = 256
ROWS = 512
C_EXP = (D ** -0.5) * math.log2(math.e)
SCALE = D ** -0.5
F32 = jnp.float32
BF16 = jnp.bfloat16


def nt(a, b):
    return lax.dot_general(a, b, (((1,), (1,)), ((), ())), preferred_element_type=F32)


def nn(a, b):
    return lax.dot_general(a, b, (((1,), (0,)), ((), ())), preferred_element_type=F32)


def kernel(q_hbm, k_hbm, v_hbm, pos_hbm, seq_hbm, qg_hbm, kg_hbm, freq_hbm, out_ref, lse_out, lay_ref,
           q_in, k_in, v_in, pos_v, seq_v, qg_v, kg_v, freq_v, f_scr, cs_scr, perm,
           kbuf, vbuf, vraw, kst, vst, qbuf, qst, kaug, m_scr, l_scr, acc, ost, obuf, lst, lbuf, pbuf, abuf,
           in_sem, ready, s_raw, r_raw, r_own, r_share, r_k, r_far, r_o, r_l):
    me = lax.axis_index("cp")
    core = lax.rem(me, 2)
    chip = lax.div(me, 2)
    x = lax.rem(chip, 2)
    y = lax.div(chip, 2)
    xchip = chip + 1 - 2 * x
    ychip = chip + 2 - 4 * y
    other = 1 - core
    partner = 2 * chip + other

    def rcopy(src, dst, ssem, rsem, dev):
        return pltpu.make_async_remote_copy(src_ref=src, dst_ref=dst, send_sem=ssem, recv_sem=rsem,
                                            device_id={"cp": dev}, device_id_type=pl.DeviceIdType.MESH)

    s_k, s_own, s_share, s_fwd, s_o, s_l = (in_sem.at[n] for n in (1, 2, 3, 4, 5, 0))

    def sized(kib):
        return kbuf.at[pl.ds(0, kib // 256)] if kib >= 256 else kbuf.at[0, pl.ds(0, kib // 128)]

    def sent(sem, kib):
        rcopy(sized(kib), sized(kib), sem, r_l.at[0], partner).wait_send()

    def arrived(sem, kib):
        rcopy(sized(kib), sized(kib), s_l, sem, partner).wait_recv()

    barrier = pltpu.get_barrier_semaphore()
    for peer in (2 * xchip + 1 - y, 2 * ychip + 1 - y, partner):
        pl.semaphore_signal(barrier, inc=1, device_id={"cp": peer}, device_id_type=pl.DeviceIdType.MESH)

    ins = [(v_hbm, v_in), (seq_hbm, seq_v), (pos_hbm, pos_v), (k_hbm, k_in), (kg_hbm, kg_v), (freq_hbm, freq_v),
           (q_hbm, q_in), (qg_hbm, qg_v)]
    in_copies = [pltpu.make_async_copy(src, dst, in_sem.at[n]) for n, (src, dst) in enumerate(ins)]
    for n in (1, 2, 5, 3, 4, 0, 6, 7):
        in_copies[n].start()

    pl.semaphore_wait(barrier, 3)
    pl.semaphore_signal(ready, inc=1, device_id={"cp": partner}, device_id_type=pl.DeviceIdType.MESH)

    def raw_v(t):
        tchip = xchip + t * (ychip - xchip)
        return rcopy(v_hbm, vraw.at[t], s_raw.at[0], r_raw.at[t], 2 * tchip + core)

    first = 1 - (core + y - 2 * core * y)
    raw_v(first).start()
    pl.semaphore_wait(ready, 1)
    raw_v(1 - first).start()

    in_copies[1].wait()
    seq = seq_v[...]
    row_id = lax.broadcasted_iota(jnp.int32, (8, ROWS), 1).astype(F32)
    sub_id = lax.broadcasted_iota(jnp.int32, (8, ROWS), 0)
    is_seq = jnp.broadcast_to(seq, (8, ROWS)) == sub_id
    seq_f = jnp.where(is_seq, 1.0, 0.0)
    cnt = jnp.sum(seq_f, axis=1, keepdims=True)
    start = jnp.min(jnp.where(is_seq, row_id, float(ROWS)), axis=1, keepdims=True)
    start_row = jnp.sum(seq_f * start, axis=0, keepdims=True)
    cnt_row = jnp.sum(seq_f * cnt, axis=0, keepdims=True)
    off = row_id[:1] - start_row
    late = off * 2.0 >= cnt_row
    dest = start_row * 0.5 + off + jnp.where(late, HALF - 0.5 * cnt_row, 0.0)
    dest_i = dest.astype(jnp.int32)
    for blk in range(4):
        rows = lax.broadcasted_iota(jnp.int32, (128, ROWS), 0) + blk * 128
        perm[pl.ds(blk * 128, 128), :] = jnp.where(rows == dest_i, 1.0, 0.0).astype(BF16)

    def send_k(half):
        for h in range(2):
            for t, tchip in enumerate((xchip, ychip)):
                rcopy(kst.at[h, half], kbuf.at[1 + t, core, half], s_k, r_k.at[t, half], 2 * tchip + h).start()

    def split_v(src, slot):
        f_scr[pl.ds(0, 2 * ROWS), :] = src[...].astype(F32)
        for mine in range(2):
            h = core if mine else other
            vt = f_scr[pl.ds(h, ROWS, stride=2), :].T.astype(BF16)
            vc = nt(vt, perm[...]).astype(BF16)
            for half in range(2):
                part = vc[:, half * HALF:(half + 1) * HALF]
                if mine:
                    vbuf[slot, core, half] = part
                else:
                    vst[slot, half] = part
        rcopy(vst.at[slot], vbuf.at[slot, core], s_share if slot else s_own, r_share.at[0] if slot else r_own.at[0], partner).start()

    in_copies[2].wait()
    in_copies[5].wait()
    angle = freq_v[...] * pos_v[...].astype(F32)
    cs_scr[0] = jnp.cos(angle)
    cs_scr[1] = jnp.sin(angle)

    def norm_rope(rows_f32, gain_v):
        xt = rows_f32.T
        inv = lax.rsqrt(jnp.mean(xt * xt, axis=0, keepdims=True) + EPS)
        gain = jnp.broadcast_to(gain_v[...].astype(F32), (128, D)).T
        gain = jnp.concatenate([gain] * 4, axis=1)
        n = (xt * inv * gain).astype(BF16).astype(F32)
        a, b = n[:64], n[64:]
        cos, sin = cs_scr[0], cs_scr[1]
        return jnp.concatenate([a * cos - b * sin, b * cos + a * sin], axis=0).astype(BF16)

    in_copies[3].wait()
    in_copies[4].wait()
    f_scr[pl.ds(0, 1024), :] = k_in[...].astype(F32)
    for h in range(2):
        kr = norm_rope(f_scr[pl.ds(h, ROWS, stride=2), :], kg_v)
        kc = nt(perm[...], kr).astype(BF16)
        for half in range(2):
            kst[h, half] = kc[half * HALF:(half + 1) * HALF, :]
    for half in range(2):
        kbuf[0, core, half] = kst[core, half]

    send_k(0)
    send_k(1)
    rcopy(kst.at[other], kbuf.at[0, core], s_own, r_own.at[0], partner).start()

    in_copies[0].wait()
    split_v(v_in, 0)

    in_copies[6].wait()
    in_copies[7].wait()
    f_scr[...] = q_in[...].astype(F32)

    def q_head(h, store):
        qr = norm_rope(f_scr[pl.ds(h, ROWS, stride=4), :], qg_v)
        qc = nt(qr, perm[...]).astype(BF16)
        for half in range(2):
            store(half, qc[:, half * HALF:(half + 1) * HALF])

    for g in range(2):
        def store_other(half, val, g=g):
            qst[half, :, g * HALF:(g + 1) * HALF] = val
        q_head(2 * other + g, store_other)
    rcopy(qst, qbuf.at[:, 0, pl.ds(0, D), :], s_own, r_own.at[0], partner).start()
    for g in range(2):
        def store_own(half, val, g=g):
            qbuf[half, 1, pl.ds(0, D), g * HALF:(g + 1) * HALF] = val
        q_head(2 * core + g, store_own)

    lane_d = lax.broadcasted_iota(jnp.int32, (8, HALF), 1).astype(F32)
    in_run = (lane_d >= start * 0.5) & (lane_d < (start + cnt) * 0.5)
    one_hot = jnp.where(in_run, 1.0, 0.0)
    blocked = jnp.where(in_run, 0.0, NEG_BIG)
    blocked = jnp.where(lax.broadcasted_iota(jnp.int32, (8, HALF), 0) < 4, blocked, 0.0)
    pad = jnp.zeros((D - 8, HALF), F32)
    q_extra = jnp.concatenate([blocked, pad], axis=0).astype(BF16)
    for half in range(2):
        for dev in range(2):
            for g in range(2):
                qbuf[half, dev, pl.ds(D, D), g * HALF:(g + 1) * HALF] = q_extra
    kaug[...] = jnp.concatenate([one_hot, pad], axis=0).T.astype(BF16)

    lane_l = lax.broadcasted_iota(jnp.int32, (8, D), 1)
    lay_ref[...] = jnp.where(lane_l == 0, start, cnt * 0.5).astype(jnp.int32)

    m_scr[...] = jnp.full(m_scr.shape, NEG_BIG, F32)
    l_scr[...] = jnp.zeros(l_scr.shape, F32)
    acc[...] = jnp.zeros(acc.shape, F32)

    def tile_parts(slot, khalf, qhalf, causal):
        ka = kaug[...]
        keys = [jnp.concatenate([kbuf[slot, dev, khalf], ka], axis=1) for dev in range(2)]
        keys = jnp.concatenate(keys, axis=0)
        v0 = vbuf[slot, 0, khalf]
        v1 = vbuf[slot, 1, khalf]
        chunks = [(dev, g) for dev in range(2) for g in range(2)]

        def scores(n):
            dev, g = chunks[n]
            s = nn(keys, qbuf[qhalf, dev, :, pl.ds(g * HALF, HALF)])
            if causal:
                abs_dev = core if dev == 1 else other
                krow = lax.broadcasted_iota(jnp.int32, (2 * HALF, HALF), 0)
                qcol = lax.broadcasted_iota(jnp.int32, (2 * HALF, HALF), 1)
                kord = krow + qhalf * jnp.where(krow < HALF, HALF, -HALF)
                qord = qcol + (abs_dev + qhalf * (1 - 2 * abs_dev)) * HALF
                s = jnp.where(kord <= qord, s, NEG_BIG)
            return s

        def soft(n, s):
            dev, g = chunks[n]
            cols = pl.ds(g * HALF, HALF)
            m_old = m_scr[qhalf, dev, :, cols]
            m_new = jnp.maximum(m_old, jnp.max(s, axis=0, keepdims=True))
            p = jnp.exp2((s - m_new) * C_EXP)
            alpha = jnp.exp2((m_old - m_new) * C_EXP)
            m_scr[qhalf, dev, :, cols] = m_new
            l_scr[qhalf, dev, :, cols] = l_scr[qhalf, dev, :, cols] * alpha + jnp.sum(p, axis=0, keepdims=True)
            return p.astype(BF16), alpha

        def out(n, pb, alpha):
            dev, g = chunks[n]
            cols = pl.ds(g * HALF, HALF)
            o = nn(v0, pb[:HALF]) + nn(v1, pb[HALF:])
            acc[qhalf, dev, :, cols] = acc[qhalf, dev, :, cols] * alpha + o

        return scores, soft, out

    def tile(slot, khalf, qhalf, causal):
        scores, soft, out = tile_parts(slot, khalf, qhalf, causal)
        s = scores(0)
        prev = None
        for n in range(4):
            nxt = scores(n + 1) if n < 3 else None
            pb, alpha = soft(n, s)
            if prev is not None:
                out(n - 1, *prev)
            prev = (pb, alpha)
            s = nxt
        out(3, *prev)

    arrived(r_own.at[0], 512)

    def own_body(half, carry):
        tile(0, half, half, True)
        return carry

    lax.fori_loop(0, 2, own_body, 0)

    def fwd_v(dev, half):
        slot, to = (2, xchip) if dev == 0 else (1, ychip)
        return rcopy(vbuf.at[slot, dev, half], vbuf.at[3, dev, half], s_fwd, r_far.at[half, 1], 2 * to + core)

    def fwd_k(dev, half):
        slot, to = (2, xchip) if dev == 0 else (1, ychip)
        return rcopy(kbuf.at[slot, dev, half], kbuf.at[3, dev, half], s_fwd, r_far.at[half, 0], 2 * to + core)

    done = y
    last = 1 - y

    def place(grp, half):
        for g in range(2):
            f_scr[pl.ds(half * 4 * HALF + 2 * grp + g, HALF, stride=4), :] = obuf[grp, half, g].astype(F32)

    def pack(half):
        rows = pl.ds(pl.multiple_of(half * 4 * HALF, 4 * HALF), 4 * HALF)
        out_ref[rows, :] = f_scr[rows, :].astype(BF16)

    def give(half, n):
        return rcopy(ost.at[half], obuf.at[core, half], s_o, r_o.at[n], partner)

    def take(half, n):
        rcopy(ost.at[half], obuf.at[other, half], s_o, r_o.at[n], partner).wait_recv()

    def early(half):
        for g in range(2):
            cols = pl.ds(g * HALF, HALF)
            ost[half, g] = (acc[half, 0, :, cols] * (1.0 / l_scr[half, 0, :, cols])).T.astype(BF16)
        give(half, 0).start()
        for g in range(2):
            cols = pl.ds(g * HALF, HALF)
            obuf[core, half, g] = (acc[half, 1, :, cols] * (1.0 / l_scr[half, 1, :, cols])).T.astype(BF16)
        place(core, half)

    def take_early(half):
        take(half, 0)
        place(other, half)
        pack(half)

    def body(idx, carry):
        @pl.when(idx == 1)
        def _():
            for t in range(2):
                raw_v(t).wait_recv()
                split_v(vraw.at[t], 1 + t)
            arrived(r_share.at[0], 256)
            for t in range(2):
                arrived(r_k.at[t, 0], 128)
                fwd_k(1 - t, 0).start()
            for dev in range(2):
                fwd_v(dev, 0).start()

        @pl.when(idx == 3)
        def _():
            for t in range(2):
                arrived(r_k.at[t, 1], 128)
                fwd_k(1 - t, 1).start()
            for dev in range(2):
                fwd_v(dev, 1).start()

        @pl.when((idx == 4) & (y == 0))
        def _():
            early(0)

        second = idx // 3
        slot = idx - 2 * second
        late_needed = (1 - y) + (idx % 2) * (y - x)
        sel = second * late_needed
        tile(slot, sel, 1 - second + sel, False)
        return carry

    lax.fori_loop(0, 5, body, 0)

    def weigh(khalf, qhalf):
        scores, soft, _ = tile_parts(3, khalf, qhalf, False)
        s = scores(0)
        for n in range(4):
            nxt = scores(n + 1) if n < 3 else None
            pb, alpha = soft(n, s)
            pbuf[n] = pb
            abuf[n] = alpha
            s = nxt

    def weighted(n, khalf):
        return nn(vbuf[3, 0, khalf], pbuf[n, :HALF, :]) + nn(vbuf[3, 1, khalf], pbuf[n, HALF:, :])

    @pl.when(y == 0)
    def _():
        take_early(0)

    arrived(r_far.at[0, 0], 128)
    weigh(0, 1)
    arrived(r_far.at[0, 1], 128)
    for n in range(4):
        cols = pl.ds((n % 2) * HALF, HALF)
        acc[1, n // 2, :, cols] = acc[1, n // 2, :, cols] * abuf[n] + weighted(n, 0)

    @pl.when(y == 1)
    def _():
        early(1)

    @pl.when(y == 0)
    def _():
        arrived(r_far.at[1, 0], 128)

    weigh(last, last)
    for dev in range(2):
        for half in range(2):
            for g in range(2):
                cols = pl.ds(g * HALF, HALF)
                val = m_scr[half, dev, :, cols] * SCALE + jnp.log(l_scr[half, dev, :, cols])
                if dev == 0:
                    lst[pl.ds(g, 1), half * HALF:(half + 1) * HALF] = val
                else:
                    lbuf[core, pl.ds(g, 1), half * HALF:(half + 1) * HALF] = val
        if dev == 0:
            l_send = rcopy(lst, lbuf.at[core], s_l, r_l.at[0], partner)
            l_send.start()
    @pl.when(y == 1)
    def _():
        take_early(1)

    @pl.when(y == 0)
    def _():
        arrived(r_far.at[1, 1], 128)

    for n in range(4):
        cols = pl.ds((n % 2) * HALF, HALF)
        dev, g = n // 2, n % 2
        o = ((acc[last, dev, :, cols] * abuf[n] + weighted(n, last)) * (1.0 / l_scr[last, dev, :, cols])).T.astype(BF16)
        if dev == 0:
            ost[last, g] = o
        else:
            obuf[core, last, g] = o
        if n == 1:
            give(last, 1).start()
    place(core, last)
    rcopy(lst, lbuf.at[other], s_l, r_l.at[0], partner).wait_recv()
    lse = jnp.concatenate([lbuf[0, :2], lbuf[1, :2]], axis=0)
    hi = lse.astype(BF16).astype(F32)
    rest = lse - hi
    mid = rest.astype(BF16).astype(F32)
    pieces = jnp.concatenate([hi, mid, rest - mid, jnp.zeros((4, ROWS), F32)], axis=0).astype(BF16)
    pieces = nn(pieces, perm[...])
    lse_out[...] = pieces[0:4] + pieces[4:8] + pieces[8:12]
    for sem, kib in ((s_raw.at[0], 512), (s_k, 512), (s_own, 512), (s_share, 256), (s_fwd, 512)):
        sent(sem, kib)
    l_send.wait_send()
    @pl.when(y == 1)
    def _():
        for n in range(2):
            arrived(r_far.at[1, n], 128)

    take(last, 1)
    place(other, last)
    pack(last)

    sent(s_o, 256)


def write_out(o_ref, l_ref, lay_ref, o_hbm, l_hbm, sem):
    lse_copy = pltpu.make_async_copy(l_ref, l_hbm, sem.at[1])
    lse_copy.start()
    lay = lay_ref[...]
    for seq in range(4):
        first, piece = lay[seq, 0], lay[seq, 1]
        for half in range(2):
            src = o_ref.at[pl.ds(half * HALF + first // 2, piece)]
            pltpu.make_async_copy(src, o_hbm.at[pl.ds(first + half * piece, piece)], sem.at[0]).start()
    pltpu.make_async_copy(o_ref, o_hbm, sem.at[0]).wait()
    lse_copy.wait()


def solution(mesh):
    freq = (THETA ** (-(np.arange(64, dtype=np.float64) * 2.0) / D)).astype(np.float32)
    freq = np.broadcast_to(freq[:, None], (64, ROWS)).copy()
    any_spec = pl.BlockSpec(memory_space=pl.ANY)
    dma = pltpu.SemaphoreType.DMA
    vm = pltpu.VMEM

    def per_device(q_raw, k_raw, v_raw, positions, seq_ids, q_gain, k_gain):
        call = pl.pallas_call(
            kernel,
            out_shape=(jax.ShapeDtypeStruct((4 * ROWS, D), BF16), jax.ShapeDtypeStruct((4, ROWS), F32), jax.ShapeDtypeStruct((8, D), jnp.int32)),
            in_specs=[any_spec] * 8,
            out_specs=(pl.BlockSpec(memory_space=pltpu.VMEM),) * 3,
            scratch_shapes=[
                vm((4 * ROWS, D), BF16), vm((2 * ROWS, D), BF16), vm((2 * ROWS, D), BF16),
                vm((1, ROWS), jnp.int32), vm((1, ROWS), jnp.int32), vm((1, D), BF16), vm((1, D), BF16),
                vm((64, ROWS), F32),
                vm((4 * ROWS, D), F32), vm((2, 64, ROWS), F32), vm((ROWS, ROWS), BF16),
                vm((4, 2, 2, HALF, D), BF16), vm((4, 2, 2, D, HALF), BF16),
                vm((2, 2 * ROWS, D), BF16), vm((2, 2, HALF, D), BF16), vm((3, 2, D, HALF), BF16),
                vm((2, 2, 2 * D, 2 * HALF), BF16), vm((2, D, 2 * HALF), BF16), vm((HALF, D), BF16),
                vm((2, 2, 1, 2 * HALF), F32), vm((2, 2, 1, 2 * HALF), F32), vm((2, 2, D, 2 * HALF), F32),
                vm((2, 2, HALF, D), BF16), vm((2, 2, 2, HALF, D), BF16), vm((8, ROWS), F32), vm((2, 8, ROWS), F32),
                vm((4, 2 * HALF, HALF), BF16), vm((4, 1, HALF), F32),
                dma((8,)), pltpu.SemaphoreType.REGULAR, dma((1,)), dma((2,)), dma((1,)), dma((1,)), dma((2, 2)), dma((2, 2)), dma((2,)), dma((1,)),
            ],
            compiler_params=pltpu.CompilerParams(collective_id=0, has_side_effects=True, vmem_limit_bytes=40000 * 1024),
        )
        args = (q_raw.reshape(4 * ROWS, D), k_raw.reshape(2 * ROWS, D), v_raw.reshape(2 * ROWS, D),
                positions.reshape(1, ROWS), seq_ids.reshape(1, ROWS), q_gain.reshape(1, D), k_gain.reshape(1, D),
                jnp.asarray(freq))
        args = [pltpu.with_memory_space_constraint(a, pltpu.HBM) for a in args]
        out, lse, lay = call(*args)
        out, lse = pl.pallas_call(
            write_out,
            out_shape=(jax.ShapeDtypeStruct((ROWS, 4, D), BF16), jax.ShapeDtypeStruct((4, ROWS), F32)),
            in_specs=[pl.BlockSpec(memory_space=pltpu.VMEM)] * 3,
            out_specs=(pl.BlockSpec(memory_space=pltpu.HBM), pl.BlockSpec(memory_space=pltpu.HBM)),
            scratch_shapes=[dma((2,))],
            compiler_params=pltpu.CompilerParams(vmem_limit_bytes=1024 * 1024),
        )(out.reshape(ROWS, 4, D), lse, lay)
        return out, lse.T

    return jax.shard_map(per_device, mesh=mesh, in_specs=(P("cp", "tp", None), P("cp", "tp", None), P("cp", "tp", None), P("cp"), P("cp"), P(), P()), out_specs=(P("cp", "tp", None), P("cp", "tp")), check_vma=False)
```

```python
import math

import jax
import jax.numpy as jnp
import numpy as np
from jax import lax
from jax.experimental import pallas as pl
from jax.experimental.pallas import tpu as pltpu
from jax.sharding import PartitionSpec as P

THETA = 1000000.0
EPS = 1e-6
NEG_BIG = -1e30
D = 128
HALF = 256
ROWS = 512
C_EXP = (D ** -0.5) * math.log2(math.e)
SCALE = D ** -0.5
F32 = jnp.float32
BF16 = jnp.bfloat16


def nt(a, b):
    return lax.dot_general(a, b, (((1,), (1,)), ((), ())), preferred_element_type=F32)


def nn(a, b):
    return lax.dot_general(a, b, (((1,), (0,)), ((), ())), preferred_element_type=F32)


def kernel(q_hbm, k_hbm, v_hbm, pos_hbm, seq_hbm, qg_hbm, kg_hbm, freq_hbm, out_ref, lse_out, lay_ref,
           q_in, k_in, v_in, pos_v, seq_v, qg_v, kg_v, freq_v, f_scr, cs_scr, perm,
           kbuf, vbuf, vraw, kst, vst, qbuf, qst, kaug, m_scr, l_scr, acc, ost, obuf, lst, lbuf, pbuf, abuf,
           in_sem, ready, s_raw, r_raw, r_own, r_share, r_k, r_far, r_o, r_l):
    me = lax.axis_index("cp")
    core = lax.rem(me, 2)
    chip = lax.div(me, 2)
    x = lax.rem(chip, 2)
    y = lax.div(chip, 2)
    xchip = chip + 1 - 2 * x
    ychip = chip + 2 - 4 * y
    other = 1 - core
    partner = 2 * chip + other

    def rcopy(src, dst, ssem, rsem, dev):
        return pltpu.make_async_remote_copy(src_ref=src, dst_ref=dst, send_sem=ssem, recv_sem=rsem,
                                            device_id={"cp": dev}, device_id_type=pl.DeviceIdType.MESH)

    s_own, s_share, s_fwd, s_k, s_o = (in_sem.at[n] for n in range(5))

    def sized(kib):
        return f_scr.at[pl.ds(0, 2 * kib)]

    def sent(sem, kib):
        rcopy(sized(kib), sized(kib), sem, r_l.at[0], partner).wait_send()

    def arrived(sem, kib):
        rcopy(sized(kib), sized(kib), s_o, sem, partner).wait_recv()

    barrier = pltpu.get_barrier_semaphore()
    for peer in (2 * xchip + 1 - y, 2 * ychip + 1 - y, partner):
        pl.semaphore_signal(barrier, inc=1, device_id={"cp": peer}, device_id_type=pl.DeviceIdType.MESH)

    ins = [(v_hbm, v_in), (seq_hbm, seq_v), (pos_hbm, pos_v), (k_hbm, k_in), (kg_hbm, kg_v), (freq_hbm, freq_v),
           (q_hbm, q_in), (qg_hbm, qg_v)]
    in_copies = [pltpu.make_async_copy(src, dst, in_sem.at[n]) for n, (src, dst) in zip((2, 0, 0, 1, 3, 1, 2, 4), ins)]
    for n in (1, 2, 5, 3, 4, 0, 6, 7):
        in_copies[n].start()

    pl.semaphore_wait(barrier, 3)
    pl.semaphore_signal(ready, inc=1, device_id={"cp": partner}, device_id_type=pl.DeviceIdType.MESH)

    def raw_v(t):
        tchip = xchip + t * (ychip - xchip)
        return rcopy(v_hbm, vraw.at[t], s_raw.at[0], r_raw.at[0], 2 * tchip + core)

    first = 1 - (core + y - 2 * core * y)
    raw_v(first).start()
    pl.semaphore_wait(ready, 1)
    raw_v(1 - first).start()

    arrived(in_sem.at[0], 4)
    seq = seq_v[...]
    row_id = lax.broadcasted_iota(jnp.int32, (8, ROWS), 1).astype(F32)
    sub_id = lax.broadcasted_iota(jnp.int32, (8, ROWS), 0)
    is_seq = jnp.broadcast_to(seq, (8, ROWS)) == sub_id
    seq_f = jnp.where(is_seq, 1.0, 0.0)
    cnt = jnp.sum(seq_f, axis=1, keepdims=True)
    start = jnp.min(jnp.where(is_seq, row_id, float(ROWS)), axis=1, keepdims=True)
    start_row = jnp.sum(seq_f * start, axis=0, keepdims=True)
    cnt_row = jnp.sum(seq_f * cnt, axis=0, keepdims=True)
    off = row_id[:1] - start_row
    late = off * 2.0 >= cnt_row
    dest = start_row * 0.5 + off + jnp.where(late, HALF - 0.5 * cnt_row, 0.0)
    dest_i = dest.astype(jnp.int32)
    for blk in range(4):
        rows = lax.broadcasted_iota(jnp.int32, (128, ROWS), 0) + blk * 128
        perm[pl.ds(blk * 128, 128), :] = jnp.where(rows == dest_i, 1.0, 0.0).astype(BF16)

    def send_k(half):
        for h in range(2):
            for t, tchip in enumerate((xchip, ychip)):
                rcopy(kst.at[h, half], kbuf.at[1 + t, core, half], s_k, r_k.at[t, half], 2 * tchip + h).start()

    def split_v(src, slot):
        f_scr[pl.ds(0, 2 * ROWS), :] = src[...].astype(F32)
        for mine in range(2):
            h = core if mine else other
            vt = f_scr[pl.ds(h, ROWS, stride=2), :].T.astype(BF16)
            vc = nt(vt, perm[...]).astype(BF16)
            for half in range(2):
                part = vc[:, half * HALF:(half + 1) * HALF]
                if mine:
                    vbuf[slot, core, half] = part
                else:
                    vst[slot, half] = part
        rcopy(vst.at[slot], vbuf.at[slot, core], s_share if slot else s_own, r_share.at[0] if slot else r_own.at[0], partner).start()

    arrived(in_sem.at[1], 384)
    angle = freq_v[...] * pos_v[...].astype(F32)
    cs_scr[0] = jnp.cos(angle)
    cs_scr[1] = jnp.sin(angle)

    def norm_rope(rows_f32, gain_v):
        xt = rows_f32.T
        inv = lax.rsqrt(jnp.mean(xt * xt, axis=0, keepdims=True) + EPS)
        gain = jnp.broadcast_to(gain_v[...].astype(F32), (128, D)).T
        gain = jnp.concatenate([gain] * 4, axis=1)
        n = (xt * inv * gain).astype(BF16).astype(F32)
        a, b = n[:64], n[64:]
        cos, sin = cs_scr[0], cs_scr[1]
        return jnp.concatenate([a * cos - b * sin, b * cos + a * sin], axis=0).astype(BF16)

    in_copies[4].wait()
    f_scr[pl.ds(0, 1024), :] = k_in[...].astype(F32)
    for h in range(2):
        kr = norm_rope(f_scr[pl.ds(h, ROWS, stride=2), :], kg_v)
        kc = nt(perm[...], kr).astype(BF16)
        for half in range(2):
            kst[h, half] = kc[half * HALF:(half + 1) * HALF, :]
    for half in range(2):
        kbuf[0, core, half] = kst[core, half]

    send_k(0)
    send_k(1)
    rcopy(kst.at[other], kbuf.at[0, core], s_own, r_own.at[0], partner).start()

    arrived(in_sem.at[2], 768)
    split_v(v_in, 0)

    in_copies[7].wait()
    f_scr[...] = q_in[...].astype(F32)

    def q_head(h, store):
        qr = norm_rope(f_scr[pl.ds(h, ROWS, stride=4), :], qg_v)
        qc = nt(qr, perm[...]).astype(BF16)
        for half in range(2):
            store(half, qc[:, half * HALF:(half + 1) * HALF])

    for g in range(2):
        def store_other(half, val, g=g):
            qst[half, :, g * HALF:(g + 1) * HALF] = val
        q_head(2 * other + g, store_other)
    rcopy(qst, qbuf.at[:, 0, pl.ds(0, D), :], s_own, r_own.at[0], partner).start()
    for g in range(2):
        def store_own(half, val, g=g):
            qbuf[half, 1, pl.ds(0, D), g * HALF:(g + 1) * HALF] = val
        q_head(2 * core + g, store_own)

    lane_d = lax.broadcasted_iota(jnp.int32, (8, HALF), 1).astype(F32)
    in_run = (lane_d >= start * 0.5) & (lane_d < (start + cnt) * 0.5)
    one_hot = jnp.where(in_run, 1.0, 0.0)
    blocked = jnp.where(in_run, 0.0, NEG_BIG)
    blocked = jnp.where(lax.broadcasted_iota(jnp.int32, (8, HALF), 0) < 4, blocked, 0.0)
    pad = jnp.zeros((D - 8, HALF), F32)
    q_extra = jnp.concatenate([blocked, pad], axis=0).astype(BF16)
    for half in range(2):
        for dev in range(2):
            for g in range(2):
                qbuf[half, dev, pl.ds(D, D), g * HALF:(g + 1) * HALF] = q_extra
    kaug[...] = jnp.concatenate([one_hot, pad], axis=0).T.astype(BF16)

    lane_l = lax.broadcasted_iota(jnp.int32, (8, D), 1)
    lay_ref[...] = jnp.where(lane_l == 0, start, cnt * 0.5).astype(jnp.int32)

    m_scr[...] = jnp.full(m_scr.shape, NEG_BIG, F32)
    l_scr[...] = jnp.zeros(l_scr.shape, F32)
    acc[...] = jnp.zeros(acc.shape, F32)

    def tile_parts(slot, khalf, qhalf, causal):
        ka = kaug[...]
        keys = [jnp.concatenate([kbuf[slot, dev, khalf], ka], axis=1) for dev in range(2)]
        keys = jnp.concatenate(keys, axis=0)
        v0 = vbuf[slot, 0, khalf]
        v1 = vbuf[slot, 1, khalf]
        chunks = [(dev, g) for dev in range(2) for g in range(2)]

        def scores(n):
            dev, g = chunks[n]
            s = nn(keys, qbuf[qhalf, dev, :, pl.ds(g * HALF, HALF)])
            if causal:
                abs_dev = core if dev == 1 else other
                krow = lax.broadcasted_iota(jnp.int32, (2 * HALF, HALF), 0)
                qcol = lax.broadcasted_iota(jnp.int32, (2 * HALF, HALF), 1)
                kord = krow + qhalf * jnp.where(krow < HALF, HALF, -HALF)
                qord = qcol + (abs_dev + qhalf * (1 - 2 * abs_dev)) * HALF
                s = jnp.where(kord <= qord, s, NEG_BIG)
            return s

        def soft(n, s):
            dev, g = chunks[n]
            cols = pl.ds(g * HALF, HALF)
            m_old = m_scr[qhalf, dev, :, cols]
            m_new = jnp.maximum(m_old, jnp.max(s, axis=0, keepdims=True))
            p = jnp.exp2((s - m_new) * C_EXP)
            alpha = jnp.exp2((m_old - m_new) * C_EXP)
            m_scr[qhalf, dev, :, cols] = m_new
            l_scr[qhalf, dev, :, cols] = l_scr[qhalf, dev, :, cols] * alpha + jnp.sum(p, axis=0, keepdims=True)
            return p.astype(BF16), alpha

        def out(n, pb, alpha):
            dev, g = chunks[n]
            cols = pl.ds(g * HALF, HALF)
            o = nn(v0, pb[:HALF]) + nn(v1, pb[HALF:])
            acc[qhalf, dev, :, cols] = acc[qhalf, dev, :, cols] * alpha + o

        return scores, soft, out

    def tile(slot, khalf, qhalf, causal):
        scores, soft, out = tile_parts(slot, khalf, qhalf, causal)
        s = scores(0)
        prev = None
        for n in range(4):
            nxt = scores(n + 1) if n < 3 else None
            pb, alpha = soft(n, s)
            if prev is not None:
                out(n - 1, *prev)
            prev = (pb, alpha)
            s = nxt
        out(3, *prev)

    arrived(r_own.at[0], 512)

    def own_body(half, carry):
        tile(0, half, half, True)
        return carry

    lax.fori_loop(0, 2, own_body, 0)

    def fwd_v(dev, half):
        slot, to = (2, xchip) if dev == 0 else (1, ychip)
        return rcopy(vbuf.at[slot, dev, half], vbuf.at[3, dev, half], s_fwd, r_far.at[half, 1], 2 * to + core)

    def fwd_k(dev, half):
        slot, to = (2, xchip) if dev == 0 else (1, ychip)
        return rcopy(kbuf.at[slot, dev, half], kbuf.at[3, dev, half], s_fwd, r_far.at[half, 0], 2 * to + core)

    done = y
    last = 1 - y

    def place(grp, half):
        for g in range(2):
            f_scr[pl.ds(half * 4 * HALF + 2 * grp + g, HALF, stride=4), :] = obuf[grp, half, g].astype(F32)

    def pack(half):
        rows = pl.ds(pl.multiple_of(half * 4 * HALF, 4 * HALF), 4 * HALF)
        out_ref[rows, :] = f_scr[rows, :].astype(BF16)

    def give(half, n):
        return rcopy(ost.at[half], obuf.at[core, half], s_o, r_o.at[n], partner)

    def take(half, n):
        rcopy(ost.at[half], obuf.at[other, half], s_o, r_o.at[n], partner).wait_recv()

    def early(half):
        for g in range(2):
            cols = pl.ds(g * HALF, HALF)
            ost[half, g] = (acc[half, 0, :, cols] * (1.0 / l_scr[half, 0, :, cols])).T.astype(BF16)
        give(half, 0).start()
        for g in range(2):
            cols = pl.ds(g * HALF, HALF)
            obuf[core, half, g] = (acc[half, 1, :, cols] * (1.0 / l_scr[half, 1, :, cols])).T.astype(BF16)
        place(core, half)

    def take_early(half):
        take(half, 0)
        place(other, half)
        pack(half)

    def body(idx, carry):
        @pl.when(idx == 1)
        def _():
            arrived(r_raw.at[0], 512)
            for t in range(2):
                split_v(vraw.at[t], 1 + t)
            arrived(r_share.at[0], 256)
            for t in range(2):
                arrived(r_k.at[t, 0], 128)
                fwd_k(1 - t, 0).start()
            for dev in range(2):
                fwd_v(dev, 0).start()

        @pl.when(idx == 3)
        def _():
            for t in range(2):
                arrived(r_k.at[t, 1], 128)
                fwd_k(1 - t, 1).start()
            for dev in range(2):
                fwd_v(dev, 1).start()

        @pl.when((idx == 4) & (y == 0))
        def _():
            early(0)

        second = idx // 3
        slot = idx - 2 * second
        late_needed = (1 - y) + (idx % 2) * (y - x)
        sel = second * late_needed
        tile(slot, sel, 1 - second + sel, False)
        return carry

    lax.fori_loop(0, 5, body, 0)

    def weigh(khalf, qhalf):
        scores, soft, _ = tile_parts(3, khalf, qhalf, False)
        s = scores(0)
        for n in range(4):
            nxt = scores(n + 1) if n < 3 else None
            pb, alpha = soft(n, s)
            pbuf[n] = pb
            abuf[n] = alpha
            s = nxt

    def weighted(n, khalf):
        return nn(vbuf[3, 0, khalf], pbuf[n, :HALF, :]) + nn(vbuf[3, 1, khalf], pbuf[n, HALF:, :])

    @pl.when(y == 0)
    def _():
        take_early(0)

    arrived(r_far.at[0, 0], 128)
    weigh(0, 1)
    arrived(r_far.at[0, 1], 128)
    for n in range(4):
        cols = pl.ds((n % 2) * HALF, HALF)
        acc[1, n // 2, :, cols] = acc[1, n // 2, :, cols] * abuf[n] + weighted(n, 0)

    @pl.when(y == 1)
    def _():
        early(1)

    @pl.when(y == 0)
    def _():
        arrived(r_far.at[1, 0], 128)

    weigh(last, last)
    for dev in range(2):
        for half in range(2):
            for g in range(2):
                cols = pl.ds(g * HALF, HALF)
                val = m_scr[half, dev, :, cols] * SCALE + jnp.log(l_scr[half, dev, :, cols])
                if dev == 0:
                    lst[pl.ds(g, 1), half * HALF:(half + 1) * HALF] = val
                else:
                    lbuf[core, pl.ds(g, 1), half * HALF:(half + 1) * HALF] = val
        if dev == 0:
            l_send = rcopy(lst, lbuf.at[core], s_o, r_l.at[0], partner)
            l_send.start()
    @pl.when(y == 1)
    def _():
        take_early(1)

    @pl.when(y == 0)
    def _():
        arrived(r_far.at[1, 1], 128)

    for n in range(4):
        cols = pl.ds((n % 2) * HALF, HALF)
        dev, g = n // 2, n % 2
        o = ((acc[last, dev, :, cols] * abuf[n] + weighted(n, last)) * (1.0 / l_scr[last, dev, :, cols])).T.astype(BF16)
        if dev == 0:
            ost[last, g] = o
        else:
            obuf[core, last, g] = o
        if n == 1:
            give(last, 1).start()
    place(core, last)
    rcopy(lst, lbuf.at[other], s_o, r_l.at[0], partner).wait_recv()
    lse = jnp.concatenate([lbuf[0, :2], lbuf[1, :2]], axis=0)
    hi = lse.astype(BF16).astype(F32)
    rest = lse - hi
    mid = rest.astype(BF16).astype(F32)
    pieces = jnp.concatenate([hi, mid, rest - mid, jnp.zeros((4, ROWS), F32)], axis=0).astype(BF16)
    pieces = nn(pieces, perm[...])
    lse_out[...] = pieces[0:4] + pieces[4:8] + pieces[8:12]
    for sem, kib in ((s_raw.at[0], 512), (s_k, 512), (s_own, 512), (s_share, 256), (s_fwd, 512)):
        sent(sem, kib)
    @pl.when(y == 1)
    def _():
        for n in range(2):
            arrived(r_far.at[1, n], 128)

    take(last, 1)
    place(other, last)
    pack(last)

    sent(s_o, 272)


def write_out(o_ref, l_ref, lay_ref, o_hbm, l_hbm, sem):
    lse_copy = pltpu.make_async_copy(l_ref, l_hbm, sem.at[1])
    lse_copy.start()
    lay = lay_ref[...]
    for seq in range(4):
        first, piece = lay[seq, 0], lay[seq, 1]
        for half in range(2):
            src = o_ref.at[pl.ds(half * HALF + first // 2, piece)]
            pltpu.make_async_copy(src, o_hbm.at[pl.ds(first + half * piece, piece)], sem.at[0]).start()
    pltpu.make_async_copy(o_ref, o_hbm, sem.at[0]).wait()
    lse_copy.wait()


def solution(mesh):
    freq = (THETA ** (-(np.arange(64, dtype=np.float64) * 2.0) / D)).astype(np.float32)
    freq = np.broadcast_to(freq[:, None], (64, ROWS)).copy()
    any_spec = pl.BlockSpec(memory_space=pl.ANY)
    dma = pltpu.SemaphoreType.DMA
    vm = pltpu.VMEM

    def per_device(q_raw, k_raw, v_raw, positions, seq_ids, q_gain, k_gain):
        call = pl.pallas_call(
            kernel,
            out_shape=(jax.ShapeDtypeStruct((4 * ROWS, D), BF16), jax.ShapeDtypeStruct((4, ROWS), F32), jax.ShapeDtypeStruct((8, D), jnp.int32)),
            in_specs=[any_spec] * 8,
            out_specs=(pl.BlockSpec(memory_space=pltpu.VMEM),) * 3,
            scratch_shapes=[
                vm((4 * ROWS, D), BF16), vm((2 * ROWS, D), BF16), vm((2 * ROWS, D), BF16),
                vm((1, ROWS), jnp.int32), vm((1, ROWS), jnp.int32), vm((1, D), BF16), vm((1, D), BF16),
                vm((64, ROWS), F32),
                vm((4 * ROWS, D), F32), vm((2, 64, ROWS), F32), vm((ROWS, ROWS), BF16),
                vm((4, 2, 2, HALF, D), BF16), vm((4, 2, 2, D, HALF), BF16),
                vm((2, 2 * ROWS, D), BF16), vm((2, 2, HALF, D), BF16), vm((3, 2, D, HALF), BF16),
                vm((2, 2, 2 * D, 2 * HALF), BF16), vm((2, D, 2 * HALF), BF16), vm((HALF, D), BF16),
                vm((2, 2, 1, 2 * HALF), F32), vm((2, 2, 1, 2 * HALF), F32), vm((2, 2, D, 2 * HALF), F32),
                vm((2, 2, HALF, D), BF16), vm((2, 2, 2, HALF, D), BF16), vm((8, ROWS), F32), vm((2, 8, ROWS), F32),
                vm((4, 2 * HALF, HALF), BF16), vm((4, 1, HALF), F32),
                dma((5,)), pltpu.SemaphoreType.REGULAR, dma((1,)), dma((1,)), dma((1,)), dma((1,)), dma((2, 2)), dma((2, 2)), dma((2,)), dma((1,)),
            ],
            compiler_params=pltpu.CompilerParams(collective_id=0, has_side_effects=True, vmem_limit_bytes=40000 * 1024),
        )
        args = (q_raw.reshape(4 * ROWS, D), k_raw.reshape(2 * ROWS, D), v_raw.reshape(2 * ROWS, D),
                positions.reshape(1, ROWS), seq_ids.reshape(1, ROWS), q_gain.reshape(1, D), k_gain.reshape(1, D),
                jnp.asarray(freq))
        args = [pltpu.with_memory_space_constraint(a, pltpu.HBM) for a in args]
        out, lse, lay = call(*args)
        out, lse = pl.pallas_call(
            write_out,
            out_shape=(jax.ShapeDtypeStruct((ROWS, 4, D), BF16), jax.ShapeDtypeStruct((4, ROWS), F32)),
            in_specs=[pl.BlockSpec(memory_space=pltpu.VMEM)] * 3,
            out_specs=(pl.BlockSpec(memory_space=pltpu.HBM), pl.BlockSpec(memory_space=pltpu.HBM)),
            scratch_shapes=[dma((2,))],
            compiler_params=pltpu.CompilerParams(vmem_limit_bytes=1024 * 1024),
        )(out.reshape(ROWS, 4, D), lse, lay)
        return out, lse.T

    return jax.shard_map(per_device, mesh=mesh, in_specs=(P("cp", "tp", None), P("cp", "tp", None), P("cp", "tp", None), P("cp"), P("cp"), P(), P()), out_specs=(P("cp", "tp", None), P("cp", "tp")), check_vma=False)
```

```python
import math

import jax
import jax.numpy as jnp
import numpy as np
from jax import lax
from jax.experimental import pallas as pl
from jax.experimental.pallas import tpu as pltpu
from jax.sharding import PartitionSpec as P

THETA = 1000000.0
EPS = 1e-6
NEG_BIG = -1e30
D = 128
HALF = 256
ROWS = 512
C_EXP = (D ** -0.5) * math.log2(math.e)
SCALE = D ** -0.5
F32 = jnp.float32
BF16 = jnp.bfloat16


def nt(a, b):
    return lax.dot_general(a, b, (((1,), (1,)), ((), ())), preferred_element_type=F32)


def nn(a, b):
    return lax.dot_general(a, b, (((1,), (0,)), ((), ())), preferred_element_type=F32)


def kernel(q_hbm, k_hbm, v_hbm, pos_hbm, seq_hbm, qg_hbm, kg_hbm, freq_hbm, out_ref, lse_out, lay_ref,
           q_in, k_in, v_in, pos_v, seq_v, qg_v, kg_v, freq_v, f_scr, cs_scr, perm,
           kbuf, vbuf, vraw, kst, vst, qbuf, qst, kaug, m_scr, l_scr, acc, ost, obuf, lst, lbuf, pbuf, abuf,
           in_sem, ready, s_raw, r_raw, r_own, r_share, r_k, r_far, r_o, r_l):
    me = lax.axis_index("cp")
    core = lax.rem(me, 2)
    chip = lax.div(me, 2)
    x = lax.rem(chip, 2)
    y = lax.div(chip, 2)
    xchip = chip + 1 - 2 * x
    ychip = chip + 2 - 4 * y
    other = 1 - core
    partner = 2 * chip + other

    def rcopy(src, dst, ssem, rsem, dev):
        return pltpu.make_async_remote_copy(src_ref=src, dst_ref=dst, send_sem=ssem, recv_sem=rsem,
                                            device_id={"cp": dev}, device_id_type=pl.DeviceIdType.MESH)

    s_own, s_share, s_fwd, s_k, s_o = (in_sem.at[n] for n in range(5))

    def sized(kib):
        return f_scr.at[pl.ds(0, 2 * kib)]

    def sent(sem, kib):
        rcopy(sized(kib), sized(kib), sem, r_l.at[0], partner).wait_send()

    def arrived(sem, kib):
        rcopy(sized(kib), sized(kib), s_o, sem, partner).wait_recv()

    barrier = pltpu.get_barrier_semaphore()
    for peer in (2 * xchip + 1 - y, 2 * ychip + 1 - y, partner):
        pl.semaphore_signal(barrier, inc=1, device_id={"cp": peer}, device_id_type=pl.DeviceIdType.MESH)

    ins = [(v_hbm, v_in), (seq_hbm, seq_v), (pos_hbm, pos_v), (k_hbm, k_in), (kg_hbm, kg_v), (freq_hbm, freq_v),
           (q_hbm, q_in), (qg_hbm, qg_v)]
    in_copies = [pltpu.make_async_copy(src, dst, in_sem.at[n]) for n, (src, dst) in zip((2, 0, 0, 1, 3, 1, 2, 4), ins)]
    for n in (1, 2, 5, 3, 4, 0, 6, 7):
        in_copies[n].start()

    pl.semaphore_wait(barrier, 3)
    pl.semaphore_signal(ready, inc=1, device_id={"cp": partner}, device_id_type=pl.DeviceIdType.MESH)

    def raw_v(t):
        tchip = xchip + t * (ychip - xchip)
        return rcopy(v_hbm, vraw.at[t], s_raw.at[0], r_raw.at[0], 2 * tchip + core)

    first = 1 - (core + y - 2 * core * y)
    raw_v(first).start()
    pl.semaphore_wait(ready, 1)
    raw_v(1 - first).start()

    arrived(in_sem.at[0], 4)
    seq = seq_v[...]
    row_id = lax.broadcasted_iota(jnp.int32, (8, ROWS), 1).astype(F32)
    sub_id = lax.broadcasted_iota(jnp.int32, (8, ROWS), 0)
    is_seq = jnp.broadcast_to(seq, (8, ROWS)) == sub_id
    seq_f = jnp.where(is_seq, 1.0, 0.0)
    cnt = jnp.sum(seq_f, axis=1, keepdims=True)
    start = jnp.min(jnp.where(is_seq, row_id, float(ROWS)), axis=1, keepdims=True)
    start_row = jnp.sum(seq_f * start, axis=0, keepdims=True)
    cnt_row = jnp.sum(seq_f * cnt, axis=0, keepdims=True)
    off = row_id[:1] - start_row
    late = off * 2.0 >= cnt_row
    dest = start_row * 0.5 + off + jnp.where(late, HALF - 0.5 * cnt_row, 0.0)
    dest_i = dest.astype(jnp.int32)
    for blk in range(4):
        rows = lax.broadcasted_iota(jnp.int32, (128, ROWS), 0) + blk * 128
        perm[pl.ds(blk * 128, 128), :] = jnp.where(rows == dest_i, 1.0, 0.0).astype(BF16)

    def send_k(half):
        for h in range(2):
            for t, tchip in enumerate((xchip, ychip)):
                rcopy(kst.at[h, half], kbuf.at[1 + t, core, half], s_k, r_k.at[t, half], 2 * tchip + h).start()

    def split_v(src, slot):
        f_scr[pl.ds(0, 2 * ROWS), :] = src[...].astype(F32)
        for mine in range(2):
            h = core if mine else other
            vt = f_scr[pl.ds(h, ROWS, stride=2), :].T.astype(BF16)
            vc = nt(vt, perm[...]).astype(BF16)
            for half in range(2):
                part = vc[:, half * HALF:(half + 1) * HALF]
                if mine:
                    vbuf[slot, core, half] = part
                else:
                    vst[slot, half] = part
        rcopy(vst.at[slot], vbuf.at[slot, core], s_share if slot else s_own, r_share.at[0] if slot else r_own.at[0], partner).start()

    arrived(in_sem.at[1], 384)
    angle = freq_v[...] * pos_v[...].astype(F32)
    cs_scr[0] = jnp.cos(angle)
    cs_scr[1] = jnp.sin(angle)

    def norm_rope(rows_f32, gain_v):
        xt = rows_f32.T
        inv = lax.rsqrt(jnp.mean(xt * xt, axis=0, keepdims=True) + EPS)
        gain = jnp.broadcast_to(gain_v[...].astype(F32), (128, D)).T
        gain = jnp.concatenate([gain] * 4, axis=1)
        n = (xt * inv * gain).astype(BF16).astype(F32)
        a, b = n[:64], n[64:]
        cos, sin = cs_scr[0], cs_scr[1]
        return jnp.concatenate([a * cos - b * sin, b * cos + a * sin], axis=0).astype(BF16)

    in_copies[4].wait()
    f_scr[pl.ds(0, 1024), :] = k_in[...].astype(F32)
    for h in range(2):
        kr = norm_rope(f_scr[pl.ds(h, ROWS, stride=2), :], kg_v)
        kc = nt(perm[...], kr).astype(BF16)
        for half in range(2):
            kst[h, half] = kc[half * HALF:(half + 1) * HALF, :]
    for half in range(2):
        kbuf[0, core, half] = kst[core, half]

    send_k(0)
    send_k(1)
    rcopy(kst.at[other], kbuf.at[0, core], s_own, r_own.at[0], partner).start()

    arrived(in_sem.at[2], 768)
    split_v(v_in, 0)

    in_copies[7].wait()
    f_scr[...] = q_in[...].astype(F32)

    def q_head(h, store):
        qr = norm_rope(f_scr[pl.ds(h, ROWS, stride=4), :], qg_v)
        qc = nt(qr, perm[...]).astype(BF16)
        for half in range(2):
            store(half, qc[:, half * HALF:(half + 1) * HALF])

    for g in range(2):
        def store_other(half, val, g=g):
            qst[half, :, g * HALF:(g + 1) * HALF] = val
        q_head(2 * other + g, store_other)
    rcopy(qst, qbuf.at[:, 0, pl.ds(0, D), :], s_own, r_own.at[0], partner).start()
    for g in range(2):
        def store_own(half, val, g=g):
            qbuf[half, 1, pl.ds(0, D), g * HALF:(g + 1) * HALF] = val
        q_head(2 * core + g, store_own)

    lane_d = lax.broadcasted_iota(jnp.int32, (8, HALF), 1).astype(F32)
    in_run = (lane_d >= start * 0.5) & (lane_d < (start + cnt) * 0.5)
    one_hot = jnp.where(in_run, 1.0, 0.0)
    blocked = jnp.where(in_run, 0.0, NEG_BIG)
    blocked = jnp.where(lax.broadcasted_iota(jnp.int32, (8, HALF), 0) < 4, blocked, 0.0)
    pad = jnp.zeros((D - 8, HALF), F32)
    q_extra = jnp.concatenate([blocked, pad], axis=0).astype(BF16)
    for half in range(2):
        for dev in range(2):
            for g in range(2):
                qbuf[half, dev, pl.ds(D, D), g * HALF:(g + 1) * HALF] = q_extra
    kaug[...] = jnp.concatenate([one_hot, pad], axis=0).T.astype(BF16)

    lane_l = lax.broadcasted_iota(jnp.int32, (8, D), 1)
    lay_ref[...] = jnp.where(lane_l == 0, start, cnt * 0.5).astype(jnp.int32)

    m_scr[...] = jnp.full(m_scr.shape, NEG_BIG, F32)
    l_scr[...] = jnp.zeros(l_scr.shape, F32)
    acc[...] = jnp.zeros(acc.shape, F32)

    def tile_parts(slot, khalf, qhalf, causal):
        ka = kaug[...]
        keys = [jnp.concatenate([kbuf[slot, dev, khalf], ka], axis=1) for dev in range(2)]
        keys = jnp.concatenate(keys, axis=0)
        v0 = vbuf[slot, 0, khalf]
        v1 = vbuf[slot, 1, khalf]
        chunks = [(dev, g) for dev in range(2) for g in range(2)]

        def scores(n):
            dev, g = chunks[n]
            s = nn(keys, qbuf[qhalf, dev, :, pl.ds(g * HALF, HALF)])
            if causal:
                abs_dev = core if dev == 1 else other
                krow = lax.broadcasted_iota(jnp.int32, (2 * HALF, HALF), 0)
                qcol = lax.broadcasted_iota(jnp.int32, (2 * HALF, HALF), 1)
                kord = krow + qhalf * jnp.where(krow < HALF, HALF, -HALF)
                qord = qcol + (abs_dev + qhalf * (1 - 2 * abs_dev)) * HALF
                s = jnp.where(kord <= qord, s, NEG_BIG)
            return s

        def soft(n, s):
            dev, g = chunks[n]
            cols = pl.ds(g * HALF, HALF)
            m_old = m_scr[qhalf, dev, :, cols]
            m_new = jnp.maximum(m_old, jnp.max(s, axis=0, keepdims=True))
            p = jnp.exp2((s - m_new) * C_EXP)
            alpha = jnp.exp2((m_old - m_new) * C_EXP)
            m_scr[qhalf, dev, :, cols] = m_new
            l_scr[qhalf, dev, :, cols] = l_scr[qhalf, dev, :, cols] * alpha + jnp.sum(p, axis=0, keepdims=True)
            return p.astype(BF16), alpha

        def out(n, pb, alpha):
            dev, g = chunks[n]
            cols = pl.ds(g * HALF, HALF)
            o = nn(v0, pb[:HALF]) + nn(v1, pb[HALF:])
            acc[qhalf, dev, :, cols] = acc[qhalf, dev, :, cols] * alpha + o

        return scores, soft, out

    def tile(slot, khalf, qhalf, causal):
        scores, soft, out = tile_parts(slot, khalf, qhalf, causal)
        s = scores(0)
        prev = None
        for n in range(4):
            nxt = scores(n + 1) if n < 3 else None
            pb, alpha = soft(n, s)
            if prev is not None:
                out(n - 1, *prev)
            prev = (pb, alpha)
            s = nxt
        out(3, *prev)

    arrived(r_own.at[0], 512)

    def own_body(half, carry):
        tile(0, half, half, True)
        return carry

    lax.fori_loop(0, 2, own_body, 0)

    def fwd_v(dev, half):
        slot, to = (2, xchip) if dev == 0 else (1, ychip)
        return rcopy(vbuf.at[slot, dev, half], vbuf.at[3, dev, half], s_fwd, r_far.at[half, 1], 2 * to + core)

    def fwd_k(dev, half):
        slot, to = (2, xchip) if dev == 0 else (1, ychip)
        return rcopy(kbuf.at[slot, dev, half], kbuf.at[3, dev, half], s_fwd, r_far.at[half, 0], 2 * to + core)

    done = y
    last = 1 - y

    def place(grp, half):
        for g in range(2):
            f_scr[pl.ds(half * 4 * HALF + 2 * grp + g, HALF, stride=4), :] = obuf[grp, half, g].astype(F32)

    def pack(half):
        rows = pl.ds(pl.multiple_of(half * 4 * HALF, 4 * HALF), 4 * HALF)
        out_ref[rows, :] = f_scr[rows, :].astype(BF16)

    def give(half, n):
        return rcopy(ost.at[half], obuf.at[core, half], s_o, r_o.at[n], partner)

    def take(half, n):
        rcopy(ost.at[half], obuf.at[other, half], s_o, r_o.at[n], partner).wait_recv()

    def early(half):
        for g in range(2):
            cols = pl.ds(g * HALF, HALF)
            ost[half, g] = (acc[half, 0, :, cols] * (1.0 / l_scr[half, 0, :, cols])).T.astype(BF16)
        give(half, 0).start()
        for g in range(2):
            cols = pl.ds(g * HALF, HALF)
            obuf[core, half, g] = (acc[half, 1, :, cols] * (1.0 / l_scr[half, 1, :, cols])).T.astype(BF16)
        place(core, half)

    def take_early(half):
        take(half, 0)
        place(other, half)
        pack(half)

    def body(idx, carry):
        @pl.when(idx == 1)
        def _():
            arrived(r_raw.at[0], 512)
            for t in range(2):
                split_v(vraw.at[t], 1 + t)
            arrived(r_share.at[0], 256)
            for t in range(2):
                arrived(r_k.at[t, 0], 128)
                fwd_k(1 - t, 0).start()
            for dev in range(2):
                fwd_v(dev, 0).start()

        @pl.when(idx == 3)
        def _():
            for t in range(2):
                arrived(r_k.at[t, 1], 128)
                fwd_k(1 - t, 1).start()
            for dev in range(2):
                fwd_v(dev, 1).start()

        @pl.when((idx == 4) & (y == 0))
        def _():
            early(0)

        second = idx // 3
        slot = idx - 2 * second
        late_needed = (1 - y) + (idx % 2) * (y - x)
        sel = second * late_needed
        tile(slot, sel, 1 - second + sel, False)
        return carry

    lax.fori_loop(0, 5, body, 0)

    def weigh(khalf, qhalf):
        scores, soft, _ = tile_parts(3, khalf, qhalf, False)
        s = scores(0)
        for n in range(4):
            nxt = scores(n + 1) if n < 3 else None
            pb, alpha = soft(n, s)
            pbuf[n] = pb
            abuf[n] = alpha
            s = nxt

    def weighted(n, khalf):
        return nn(vbuf[3, 0, khalf], pbuf[n, :HALF, :]) + nn(vbuf[3, 1, khalf], pbuf[n, HALF:, :])

    @pl.when(y == 0)
    def _():
        take_early(0)

    arrived(r_far.at[0, 0], 128)
    weigh(0, 1)
    arrived(r_far.at[0, 1], 128)
    for n in range(4):
        cols = pl.ds((n % 2) * HALF, HALF)
        acc[1, n // 2, :, cols] = acc[1, n // 2, :, cols] * abuf[n] + weighted(n, 0)

    @pl.when(y == 1)
    def _():
        early(1)

    @pl.when(y == 0)
    def _():
        arrived(r_far.at[1, 0], 128)

    weigh(last, last)
    def lse_of(dev, half, g):
        cols = pl.ds(g * HALF, HALF)
        return m_scr[half, dev, :, cols] * SCALE + jnp.log(l_scr[half, dev, :, cols])

    for half in range(2):
        for g in range(2):
            lst[pl.ds(g, 1), half * HALF:(half + 1) * HALF] = lse_of(0, half, g)
    l_send = rcopy(lst, lbuf.at[core], s_o, r_l.at[0], partner)
    l_send.start()

    @pl.when(y == 1)
    def _():
        take_early(1)

    @pl.when(y == 0)
    def _():
        arrived(r_far.at[1, 1], 128)

    for n in range(4):
        cols = pl.ds((n % 2) * HALF, HALF)
        dev, g = n // 2, n % 2
        o = ((acc[last, dev, :, cols] * abuf[n] + weighted(n, last)) * (1.0 / l_scr[last, dev, :, cols])).T.astype(BF16)
        if dev == 0:
            ost[last, g] = o
        else:
            obuf[core, last, g] = o
        if n == 1:
            give(last, 1).start()
    place(core, last)
    for half in range(2):
        for g in range(2):
            lbuf[core, pl.ds(g, 1), half * HALF:(half + 1) * HALF] = lse_of(1, half, g)
    rcopy(lst, lbuf.at[other], s_o, r_l.at[0], partner).wait_recv()
    lse = jnp.concatenate([lbuf[0, :2], lbuf[1, :2]], axis=0)
    hi = lse.astype(BF16).astype(F32)
    rest = lse - hi
    mid = rest.astype(BF16).astype(F32)
    pieces = jnp.concatenate([hi, mid, rest - mid, jnp.zeros((4, ROWS), F32)], axis=0).astype(BF16)
    pieces = nn(pieces, perm[...])
    lse_out[...] = pieces[0:4] + pieces[4:8] + pieces[8:12]
    for sem, kib in ((s_raw.at[0], 512), (s_k, 512), (s_own, 512), (s_share, 256), (s_fwd, 512)):
        sent(sem, kib)
    @pl.when(y == 1)
    def _():
        for n in range(2):
            arrived(r_far.at[1, n], 128)

    take(last, 1)
    place(other, last)
    pack(last)

    sent(s_o, 272)


def write_out(o_ref, l_ref, lay_ref, o_hbm, l_hbm, sem):
    lse_copy = pltpu.make_async_copy(l_ref, l_hbm, sem.at[1])
    lse_copy.start()
    lay = lay_ref[...]
    for seq in range(4):
        first, piece = lay[seq, 0], lay[seq, 1]
        for half in range(2):
            src = o_ref.at[pl.ds(half * HALF + first // 2, piece)]
            pltpu.make_async_copy(src, o_hbm.at[pl.ds(first + half * piece, piece)], sem.at[0]).start()
    pltpu.make_async_copy(o_ref, o_hbm, sem.at[0]).wait()
    lse_copy.wait()


def solution(mesh):
    freq = (THETA ** (-(np.arange(64, dtype=np.float64) * 2.0) / D)).astype(np.float32)
    freq = np.broadcast_to(freq[:, None], (64, ROWS)).copy()
    any_spec = pl.BlockSpec(memory_space=pl.ANY)
    dma = pltpu.SemaphoreType.DMA
    vm = pltpu.VMEM

    def per_device(q_raw, k_raw, v_raw, positions, seq_ids, q_gain, k_gain):
        call = pl.pallas_call(
            kernel,
            out_shape=(jax.ShapeDtypeStruct((4 * ROWS, D), BF16), jax.ShapeDtypeStruct((4, ROWS), F32), jax.ShapeDtypeStruct((8, D), jnp.int32)),
            in_specs=[any_spec] * 8,
            out_specs=(pl.BlockSpec(memory_space=pltpu.VMEM),) * 3,
            scratch_shapes=[
                vm((4 * ROWS, D), BF16), vm((2 * ROWS, D), BF16), vm((2 * ROWS, D), BF16),
                vm((1, ROWS), jnp.int32), vm((1, ROWS), jnp.int32), vm((1, D), BF16), vm((1, D), BF16),
                vm((64, ROWS), F32),
                vm((4 * ROWS, D), F32), vm((2, 64, ROWS), F32), vm((ROWS, ROWS), BF16),
                vm((4, 2, 2, HALF, D), BF16), vm((4, 2, 2, D, HALF), BF16),
                vm((2, 2 * ROWS, D), BF16), vm((2, 2, HALF, D), BF16), vm((3, 2, D, HALF), BF16),
                vm((2, 2, 2 * D, 2 * HALF), BF16), vm((2, D, 2 * HALF), BF16), vm((HALF, D), BF16),
                vm((2, 2, 1, 2 * HALF), F32), vm((2, 2, 1, 2 * HALF), F32), vm((2, 2, D, 2 * HALF), F32),
                vm((2, 2, HALF, D), BF16), vm((2, 2, 2, HALF, D), BF16), vm((8, ROWS), F32), vm((2, 8, ROWS), F32),
                vm((4, 2 * HALF, HALF), BF16), vm((4, 1, HALF), F32),
                dma((5,)), pltpu.SemaphoreType.REGULAR, dma((1,)), dma((1,)), dma((1,)), dma((1,)), dma((2, 2)), dma((2, 2)), dma((2,)), dma((1,)),
            ],
            compiler_params=pltpu.CompilerParams(collective_id=0, has_side_effects=True, vmem_limit_bytes=40000 * 1024),
        )
        args = (q_raw.reshape(4 * ROWS, D), k_raw.reshape(2 * ROWS, D), v_raw.reshape(2 * ROWS, D),
                positions.reshape(1, ROWS), seq_ids.reshape(1, ROWS), q_gain.reshape(1, D), k_gain.reshape(1, D),
                jnp.asarray(freq))
        args = [pltpu.with_memory_space_constraint(a, pltpu.HBM) for a in args]
        out, lse, lay = call(*args)
        out, lse = pl.pallas_call(
            write_out,
            out_shape=(jax.ShapeDtypeStruct((ROWS, 4, D), BF16), jax.ShapeDtypeStruct((4, ROWS), F32)),
            in_specs=[pl.BlockSpec(memory_space=pltpu.VMEM)] * 3,
            out_specs=(pl.BlockSpec(memory_space=pltpu.HBM), pl.BlockSpec(memory_space=pltpu.HBM)),
            scratch_shapes=[dma((2,))],
            compiler_params=pltpu.CompilerParams(vmem_limit_bytes=1024 * 1024),
        )(out.reshape(ROWS, 4, D), lse, lay)
        return out, lse.T

    return jax.shard_map(per_device, mesh=mesh, in_specs=(P("cp", "tp", None), P("cp", "tp", None), P("cp", "tp", None), P("cp"), P("cp"), P(), P()), out_specs=(P("cp", "tp", None), P("cp", "tp")), check_vma=False)
```
